256 devices in a mesh: gz: 8 (over z), gx: 4 (over x), gy: 8 (over y, core).
Axes of the slice: x: 4, y: 4, z: 8, core: 2. Of those that a mesh axis runs over, the one named last changes fastest.
Arguments:
- density: float32 [256, 1024, 1024], P('gz', 'gy', 'gx'), may hold values from 0 to 1
- mask: int32 [32, 128, 128], P('gz', 'gy', 'gx'), may hold values from 0 to 3
Outputs:
- filtered: float32 [256, 1024, 1024], P(('gz', 'gx'), 'gy')
- projected: float32 [256, 1024, 1024], P(('gz', 'gx'), 'gy')
The draws below stay inside these ranges and needn't reach their ends.
Inputs may be any that keep to these rules, and one draw needn't show every extreme that they name: `mask`: code 0 marks a void block, 1 a solid block, 2 and 3 design blocks.
All inputs are finite; a program needn't handle non-finite values.
Results may differ from the reference program's by a relative error of at most 0.0003.
Values sent between devices are 32-bit elements; how exact they have to be, the bound alone decides.
A program may use at most 128 MiB of HBM per device.

```python
import jax
import jax.numpy as jnp
from jax import lax

RADIUS = 6
CELLS = 8
NX = 1024
NY = 1024
NZ = 256


def set_ends(drawn, rng, smallest, high):
    dims = drawn.shape
    spot = [jax.random.randint(jax.random.fold_in(rng, axis), (), 0, dims[axis]) for axis in range(len(dims))]
    drawn = drawn.at[tuple(spot)].set(smallest)
    longest = dims.index(max(dims))
    spot[longest] = (spot[longest] + 1) % dims[longest]
    return drawn.at[tuple(spot)].set(high)


def steps_of(stream_key, shape, split, low, high):
    level = 1.0
    for dim, parts in split:
        steps = jax.random.uniform(jax.random.fold_in(jax.random.fold_in(stream_key, 6), dim), (parts,), jnp.float32, low / len(split), high / len(split))
        level = level * jnp.repeat(jnp.exp(steps), shape[dim] // parts).reshape((-1,) + (1,) * (len(shape) - 1 - dim))
    return level


def setup_inputs(seed: int = 0) -> dict:
    splits = jax.random.split(jax.random.key(seed), 3)
    return {
        "density": jnp.clip(1.0 * jax.random.uniform(splits[0], (NZ, NY, NX), jnp.float32) ** steps_of(splits[0], (NZ, NY, NX), ((0, 8), (1, 8), (2, 4)), -0.2, 0.2), 0.0, 1.0),
        "mask": set_ends(jax.random.randint(splits[1], (NZ // CELLS, NY // CELLS, NX // CELLS), 0, 4), jax.random.fold_in(splits[1], 1), 0, 3).astype(jnp.int32),
    }


sharpness = 8.0
threshold = 0.5


def smooth_axis(values, axis_index, count):
    widths = [(RADIUS, RADIUS) if position == axis_index else (0, 0) for position in range(values.ndim)]
    padded = jnp.pad(values, widths)
    result = jnp.zeros_like(values)
    for offset in range(-RADIUS, RADIUS + 1):
        window = lax.slice_in_dim(padded, RADIUS + offset, RADIUS + offset + count, axis=axis_index)
        result = result + float(RADIUS + 1 - abs(offset)) * window
    return result


def weight_count(count):
    return smooth_axis(jnp.ones((count,), jnp.float32), 0, count)


def reference(density, mask):
    def one_plane(item):
        plane, level = item
        block_row = mask[level // CELLS]
        design_code = jnp.repeat(jnp.repeat(block_row, CELLS, 0), CELLS, 1)
        physical = jnp.where(design_code == 0, 0.0, jnp.where(design_code == 1, 1.0, plane))
        return smooth_axis(smooth_axis(physical, 1, NX), 0, NY)

    levels = jnp.arange(NZ, dtype=jnp.int32)
    flat = lax.map(one_plane, (density, levels))
    summed = smooth_axis(flat, 0, NZ)
    counts = weight_count(NZ)[:, None, None] * weight_count(NY)[None, :, None] * weight_count(NX)[None, None, :]
    filtered = summed / counts
    top = jnp.tanh(sharpness * threshold)
    projected = (top + jnp.tanh(sharpness * (filtered - threshold))) / (top + jnp.tanh(sharpness * (1.0 - threshold)))
    return filtered, projected
```

```python
import functools
import math

import jax
import jax.numpy as jnp
from jax import lax
from jax.experimental import pallas as pl
from jax.experimental.pallas import tpu as pltpu
from jax.sharding import PartitionSpec as P

RADIUS = 6
CELLS = 8
PAD = 8
ROWS = 16

sharpness = 8.0
threshold = 0.5
top = math.tanh(sharpness * threshold)


def one_side(reach):
    return reach * (RADIUS + 1) - reach * (reach + 1) // 2


def inverse_count(position, length_all):
    reach_left = jnp.minimum(position, RADIUS)
    reach_right = jnp.minimum(length_all - 1 - position, RADIUS)
    return 1.0 / (RADIUS + 1 + one_side(reach_left) + one_side(reach_right)).astype(jnp.float32)


def iota(shape, dim):
    return lax.broadcasted_iota(jnp.int32, shape, dim)


def hat(distance):
    return jnp.maximum(RADIUS + 1 - jnp.abs(distance), 0).astype(jnp.float32)


def split(values):
    high = values.astype(jnp.bfloat16)
    return high, (values - high.astype(jnp.float32)).astype(jnp.bfloat16)


def dot(a, b):
    return jnp.dot(a, b, preferred_element_type=jnp.float32)


def kernel(sizes, density, mask, filtered, projected, field, code, edges, smooth, layers, lines,
           inv_y, inv_z, near, far, in_sem, send, recv, z_send, z_recv, y_send, y_recv):
    n_z, n_x, n_y = sizes
    planes, rows, columns = density.shape
    group = planes // n_x
    chunks = rows // ROWS
    gz, gx, gy = (lax.axis_index(a) for a in ("gz", "gx", "gy"))
    below, above = gz > 0, gz < n_z - 1
    before, after = gy > 0, gy < n_y - 1

    loads = [
        pltpu.make_async_copy(
            density.at[pl.ds(b * CELLS, CELLS)],
            field.at[pl.ds(b * CELLS, CELLS), pl.ds(PAD, rows)],
            in_sem.at[b],
        )
        for b in range(planes // CELLS)
    ]
    for load in loads:
        load.start()

    barrier = pltpu.get_barrier_semaphore()
    for d in range(1, n_x):
        pl.semaphore_signal(barrier, inc=1, device_id={"gx": lax.rem(gx + d, n_x)})
    for there, axis, peer in (
        (below, "gz", gz - 1), (above, "gz", gz + 1), (before, "gy", gy - 1), (after, "gy", gy + 1)
    ):
        @pl.when(there)
        def _():
            pl.semaphore_signal(barrier, inc=1, device_id={axis: peer})

    blocks = mask.shape[0]
    table = mask[...].astype(jnp.float32).astype(jnp.bfloat16)
    wide = jnp.where(iota((mask.shape[2], columns), 1) // CELLS == iota((mask.shape[2], columns), 0), 1.0, 0.0)
    wide = wide.astype(jnp.bfloat16)
    tall = jnp.where(iota((rows, mask.shape[1]), 0) // CELLS == iota((rows, mask.shape[1]), 1), 1.0, 0.0)
    tall = tall.astype(jnp.bfloat16)
    for b in range(blocks):
        code[b, PAD : PAD + rows, :] = dot(tall, dot(table[b], wide).astype(jnp.bfloat16))
        code[b, 0:PAD, :] = jnp.full((PAD, columns), 2.0, jnp.float32)
        code[b, PAD + rows :, :] = jnp.full((PAD, columns), 2.0, jnp.float32)
    inv_y[...] = inverse_count(gy * rows + iota(inv_y.shape, 0), n_y * rows)
    inv_z[...] = inverse_count(gz * planes + iota(inv_z.shape, 0), n_z * planes)
    square = (columns, columns)
    near[...] = hat(iota(square, 0) - iota(square, 1)).astype(jnp.bfloat16)
    source = iota(square, 0)
    source = jnp.where(source < columns // 2, source - columns // 2, source + columns // 2)
    far[...] = hat(source - iota(square, 1)).astype(jnp.bfloat16)

    @pl.when(jnp.logical_not(below))
    def _():
        smooth[0:RADIUS] = jnp.zeros((RADIUS, rows, columns), jnp.float32)

    @pl.when(jnp.logical_not(above))
    def _():
        smooth[RADIUS + planes :] = jnp.zeros((RADIUS, rows, columns), jnp.float32)

    @pl.when(jnp.logical_not(before))
    def _():
        field[:, 0:PAD, :] = jnp.zeros((planes, PAD, columns), jnp.float32)

    @pl.when(jnp.logical_not(after))
    def _():
        field[:, PAD + rows :, :] = jnp.zeros((planes, PAD, columns), jnp.float32)

    def physical(b, z, start, count):
        codes = code[b, pl.ds(start, count), :]
        return jnp.where(codes >= 1.5, field[z, pl.ds(start, count), :], codes)

    def y_copies():
        return (
            (after, before, pltpu.make_async_remote_copy(
                src_ref=edges.at[1], dst_ref=field.at[:, pl.ds(0, PAD)],
                send_sem=y_send.at[1], recv_sem=y_recv.at[1], device_id={"gy": gy + 1})),
            (before, after, pltpu.make_async_remote_copy(
                src_ref=edges.at[0], dst_ref=field.at[:, pl.ds(PAD + rows, PAD)],
                send_sem=y_send.at[0], recv_sem=y_recv.at[0], device_id={"gy": gy - 1})),
        )

    def z_up(c):
        part = pl.ds(pl.multiple_of(c * ROWS, ROWS), ROWS)
        return above, below, pltpu.make_async_remote_copy(
            src_ref=smooth.at[pl.ds(planes, RADIUS), part], dst_ref=smooth.at[pl.ds(0, RADIUS), part],
            send_sem=z_send.at[0, c], recv_sem=z_recv.at[0, c], device_id={"gz": gz + 1})

    def z_down(c):
        part = pl.ds(pl.multiple_of(c * ROWS, ROWS), ROWS)
        return below, above, pltpu.make_async_remote_copy(
            src_ref=smooth.at[pl.ds(RADIUS, RADIUS), part], dst_ref=smooth.at[pl.ds(RADIUS + planes, RADIUS), part],
            send_sem=z_send.at[1, c], recv_sem=z_recv.at[1, c], device_id={"gz": gz - 1})

    def z_copies(c):
        return z_up(c), z_down(c)

    def x_copy(g, c, source, target):
        part = pl.ds(pl.multiple_of(c * ROWS, ROWS), ROWS)
        return pltpu.make_async_remote_copy(
            src_ref=layers.at[g, :, part], dst_ref=lines.at[source, :, part],
            send_sem=send.at[c, g], recv_sem=recv.at[c, source], device_id={"gx": target})

    def along_y(c):
        start = pl.multiple_of(c * ROWS, ROWS)
        scale = jnp.concatenate([inv_y[pl.ds(start, ROWS), :]] * (columns // 128), axis=1)
        window = ROWS + 2 * PAD
        for b in range(blocks):
            def plane(i, _):
                z = b * CELLS + i
                x = physical(b, z, start, window)
                x2 = x + pltpu.roll(x, window - 1, 0)
                x4 = x2 + pltpu.roll(x2, window - 2, 0)
                x7 = x4 + (pltpu.roll(x2, window - 4, 0) + pltpu.roll(x, window - 6, 0))
                x2 = x7 + pltpu.roll(x7, 1, 0)
                x4 = x2 + pltpu.roll(x2, 2, 0)
                x7 = x4 + (pltpu.roll(x2, 4, 0) + pltpu.roll(x7, 6, 0))
                smooth[z + RADIUS, pl.ds(start, ROWS), :] = x7[PAD : PAD + ROWS] * scale
                return 0
            lax.fori_loop(0, CELLS, plane, 0, unroll=2)

    def along_z(g, c):
        def half(i, _):
            part = pl.ds(pl.multiple_of(c * ROWS + i * 8, 8), 8)
            x = [smooth[g * group + k, part, :] for k in range(group + 2 * RADIUS)]
            for _ in range(2):
                x2 = [p + q for p, q in zip(x, x[1:])]
                x4 = [p + q for p, q in zip(x2, x2[2:])]
                x = [p + (q + r) for p, q, r in zip(x4, x2[4:], x[6:])]
            own = g == gx
            for k in range(group):
                scale = jnp.concatenate([inv_z[g * group + k]] * (columns // 128), axis=1)
                x[k] = x[k] * scale

            @pl.when(own)
            def _():
                for k in range(group):
                    lines[g, k, part, :] = x[k]

            @pl.when(jnp.logical_not(own))
            def _():
                for k in range(group):
                    layers[g, k, part, :] = x[k]
            return 0
        lax.fori_loop(0, ROWS // 8, half, 0)

    def along_x(c):
        part = pl.ds(pl.multiple_of(c * ROWS, ROWS), ROWS)
        parts = []
        for s in range(n_x):
            parts.append(split(lines[s, :, part, :].reshape(group * ROWS, columns)))
        half = columns // 2
        for s in range(n_x):
            total = dot(parts[s][0], near[...]) + dot(parts[s][1], near[...])
            for j in range(2):
                if s == 0:
                    total += dot(parts[1][j][:, :half], far[half:, :])
                elif s == n_x - 1:
                    total += dot(parts[s - 1][j][:, half:], far[:half, :])
                else:
                    total += dot(jnp.concatenate([parts[s - 1][j][:, half:], parts[s + 1][j][:, :half]], axis=1), far[...])
            total = total * inverse_count(s * columns + iota((1, columns), 1), n_x * columns)
            after_tanh = 0.5 + jnp.tanh(sharpness * total - sharpness * threshold) * (0.5 / top)
            filtered[:, part, pl.ds(s * columns, columns)] = total.reshape(group, ROWS, columns)
            projected[:, part, pl.ds(s * columns, columns)] = after_tanh.reshape(group, ROWS, columns)

    for load in loads:
        load.wait()
    expected = n_x - 1 + sum(t.astype(jnp.int32) for t in (below, above, before, after))
    pl.semaphore_wait(barrier, expected)

    def start_when(copies):
        for sends, _, copy in copies:
            @pl.when(sends)
            def _():
                copy.start()

    def wait_recv_when(copies):
        for _, receives, copy in copies:
            @pl.when(receives)
            def _():
                copy.wait_recv()

    def wait_send_when(copies):
        for sends, _, copy in copies:
            @pl.when(sends)
            def _():
                copy.wait_send()

    def y_step(i):
        c = lax.rem(i + 1, chunks)

        @pl.when(i == chunks - 2)
        def _():
            wait_recv_when(y_copies())

        along_y(c)
        start_when(z_copies(c))

    def z_step(i):
        c = lax.rem(i + 1, chunks)
        for g in (*range(1, n_x - 1), 0, n_x - 1):
            if g == 0:
                wait_recv_when([z_up(c)])
            if g == n_x - 1:
                wait_recv_when([z_down(c)])
            along_z(g, c)

            @pl.when(g != gx)
            def _():
                x_copy(g, c, gx, g).start()

    def produce(i, _):
        @pl.when(i < chunks)
        def _():
            y_step(i)

        @pl.when(i == 1)
        def _():
            for b in range(blocks):
                def edge(k, _):
                    z = b * CELLS + k
                    edges[0, z] = physical(b, z, PAD, PAD)
                    edges[1, z] = physical(b, z, rows, PAD)
                    return 0
                lax.fori_loop(0, CELLS, edge, 0, unroll=4)
            start_when(y_copies())

        @pl.when(i > 0)
        def _():
            z_step(i - 1)
        return 0

    lax.fori_loop(0, chunks + 1, produce, 0)

    def consume(i, _):
        c = lax.rem(i + 1, chunks)
        for s in range(n_x):
            @pl.when(s != gx)
            def _():
                x_copy(s, c, s, s).wait_recv()
        along_x(c)
        return 0

    lax.fori_loop(0, chunks, consume, 0)

    def drain(c, _):
        wait_send_when(z_copies(c))
        for g in range(n_x):
            @pl.when(g != gx)
            def _():
                x_copy(g, c, gx, g).wait_send()
        return 0

    lax.fori_loop(0, chunks, drain, 0)
    wait_send_when(y_copies())


def solution(mesh):
    sizes = tuple(mesh.shape[a] for a in ("gz", "gx", "gy"))
    n_x = sizes[1]

    def body(density, mask):
        planes, rows, columns = density.shape
        group, chunks = planes // n_x, rows // ROWS
        out = jax.ShapeDtypeStruct((group, rows, columns * n_x), jnp.float32)
        dma = pltpu.SemaphoreType.DMA
        return pl.pallas_call(
            functools.partial(kernel, sizes),
            out_shape=(out, out),
            in_specs=[pl.BlockSpec(memory_space=pltpu.HBM), pl.BlockSpec(memory_space=pltpu.VMEM)],
            out_specs=[pl.BlockSpec(memory_space=pltpu.VMEM)] * 2,
            scratch_shapes=[
                pltpu.VMEM((planes, rows + 2 * PAD, columns), jnp.float32),
                pltpu.VMEM((planes // CELLS, rows + 2 * PAD, columns), jnp.float32),
                pltpu.VMEM((2, planes, PAD, columns), jnp.float32),
                pltpu.VMEM((planes + 2 * RADIUS, rows, columns), jnp.float32),
                pltpu.VMEM((n_x, group, rows, columns), jnp.float32),
                pltpu.VMEM((n_x, group, rows, columns), jnp.float32),
                pltpu.VMEM((rows, 128), jnp.float32),
                pltpu.VMEM((planes, 8, 128), jnp.float32),
                pltpu.VMEM((columns, columns), jnp.bfloat16),
                pltpu.VMEM((columns, columns), jnp.bfloat16),
                dma((planes // CELLS,)),
                dma((chunks, n_x)),
                dma((chunks, n_x)),
                dma((2, chunks)),
                dma((2, chunks)),
                dma((2,)),
                dma((2,)),
            ],
            compiler_params=pltpu.CompilerParams(
                collective_id=0, has_side_effects=True, vmem_limit_bytes=26 * 2**20
            ),
        )(pltpu.with_memory_space_constraint(density, pltpu.HBM), mask)

    return jax.shard_map(
        body,
        mesh=mesh,
        in_specs=(P("gz", "gy", "gx"), P("gz", "gy", "gx")),
        out_specs=(P(("gz", "gx"), "gy", None), P(("gz", "gx"), "gy", None)),
        check_vma=False,
    )
```

```python
import functools
import math

import jax
import jax.numpy as jnp
from jax import lax
from jax.experimental import pallas as pl
from jax.experimental.pallas import tpu as pltpu
from jax.sharding import PartitionSpec as P

RADIUS = 6
CELLS = 8
PAD = 8
ROWS = 16
LAG = 2

sharpness = 8.0
threshold = 0.5
top = math.tanh(sharpness * threshold)


def one_side(reach):
    return reach * (RADIUS + 1) - reach * (reach + 1) // 2


def inverse_count(position, length_all):
    reach_left = jnp.minimum(position, RADIUS)
    reach_right = jnp.minimum(length_all - 1 - position, RADIUS)
    return 1.0 / (RADIUS + 1 + one_side(reach_left) + one_side(reach_right)).astype(jnp.float32)


def iota(shape, dim):
    return lax.broadcasted_iota(jnp.int32, shape, dim)


def hat(distance):
    return jnp.maximum(RADIUS + 1 - jnp.abs(distance), 0).astype(jnp.float32)


def split(values):
    high = values.astype(jnp.bfloat16)
    return high, (values - high.astype(jnp.float32)).astype(jnp.bfloat16)


def dot(a, b):
    return jnp.dot(a, b, preferred_element_type=jnp.float32)


def along_x(lines, rows, near, far, filtered, projected, out_rows):
    n_x, planes, _, columns = lines.shape
    half = columns // 2
    parts = [split(lines[s, :, rows, :].reshape(planes * ROWS, columns)) for s in range(n_x)]
    for s in range(n_x):
        total = dot(parts[s][0], near[...]) + dot(parts[s][1], near[...])
        for j in range(2):
            if s == 0:
                total += dot(parts[1][j][:, :half], far[half:, :])
            elif s == n_x - 1:
                total += dot(parts[s - 1][j][:, half:], far[:half, :])
            else:
                total += dot(jnp.concatenate([parts[s - 1][j][:, half:], parts[s + 1][j][:, :half]], axis=1), far[...])
        total = total * inverse_count(s * columns + iota((1, columns), 1), n_x * columns)
        after_tanh = 0.5 + jnp.tanh(sharpness * total - sharpness * threshold) * (0.5 / top)
        filtered[:, out_rows, pl.ds(s * columns, columns)] = total.reshape(planes, ROWS, columns)
        projected[:, out_rows, pl.ds(s * columns, columns)] = after_tanh.reshape(planes, ROWS, columns)


def finish(lines, near, far, filtered, projected, filtered_out, projected_out, last_filtered, last_projected, sem):
    planes, rows, _ = filtered.shape
    rest = pl.ds(ROWS, rows - ROWS)
    copies = []
    for i, (source, target) in enumerate(((filtered, filtered_out), (projected, projected_out))):
        for z in range(planes):
            copies.append(pltpu.make_async_copy(source.at[z, rest], target.at[z, rest], sem.at[i, z]))
    for copy in copies:
        copy.start()
    first = pl.ds(0, ROWS)
    along_x(lines, first, near, far, last_filtered, last_projected, first)
    for i, (source, target) in enumerate(((last_filtered, filtered_out), (last_projected, projected_out))):
        copies.append(pltpu.make_async_copy(source, target.at[:, first], sem.at[i, planes]))
        copies[-1].start()
    for copy in copies:
        copy.wait()


def kernel(sizes, density, mask, filtered, projected, lines, near, far, field, table, code, edges, smooth, layers,
           inv_y, inv_z, in_sem, send, recv, z_send, z_recv, y_send, y_recv):
    n_z, n_x, n_y = sizes
    planes, rows, columns = density.shape
    group = planes // n_x
    chunks = rows // ROWS
    blocks = planes // CELLS
    free = group - RADIUS
    gz, gx, gy = (lax.axis_index(a) for a in ("gz", "gx", "gy"))
    below, above = gz > 0, gz < n_z - 1
    before, after = gy > 0, gy < n_y - 1
    outer, inner = (0, blocks - 1), tuple(range(1, blocks - 1))

    head = 3 * ROWS
    load_mask = pltpu.make_async_copy(mask, table, in_sem.at[2, 0])

    def load(part, b):
        start, count = ((0, head), (head, rows - head))[part]
        return pltpu.make_async_copy(
            density.at[pl.ds(b * CELLS, CELLS), pl.ds(start, count)],
            field.at[pl.ds(b * CELLS, CELLS), pl.ds(PAD + start, count)],
            in_sem.at[part, b],
        )

    load_mask.start()
    for part in range(2):
        for b in (*outer, *inner):
            load(part, b).start()

    barrier = pltpu.get_barrier_semaphore()
    for d in range(1, n_x):
        pl.semaphore_signal(barrier, inc=1, device_id={"gx": lax.rem(gx + d, n_x)})
    for there, axis, peer in (
        (below, "gz", gz - 1), (above, "gz", gz + 1), (before, "gy", gy - 1), (after, "gy", gy + 1)
    ):
        @pl.when(there)
        def _():
            pl.semaphore_signal(barrier, inc=1, device_id={axis: peer})

    inv_y[...] = inverse_count(gy * rows + iota(inv_y.shape, 0), n_y * rows)
    inv_z[...] = inverse_count(gz * planes + iota(inv_z.shape, 0), n_z * planes)

    @pl.when(jnp.logical_not(below))
    def _():
        smooth[0:RADIUS] = jnp.zeros((RADIUS, rows, columns), jnp.float32)

    @pl.when(jnp.logical_not(above))
    def _():
        smooth[RADIUS + planes :] = jnp.zeros((RADIUS, rows, columns), jnp.float32)

    @pl.when(jnp.logical_not(before))
    def _():
        field[:, 0:PAD, :] = jnp.zeros((planes, PAD, columns), jnp.float32)

    @pl.when(jnp.logical_not(after))
    def _():
        field[:, PAD + rows :, :] = jnp.zeros((planes, PAD, columns), jnp.float32)

    wide = jnp.where(iota((mask.shape[2], columns), 1) // CELLS == iota((mask.shape[2], columns), 0), 1.0, 0.0)
    wide = wide.astype(jnp.bfloat16)
    y_blocks = rows // CELLS
    load_mask.wait()
    for b in range(blocks):
        code[b, 0:8, :] = jnp.full((8, columns), 2.0, jnp.float32)
        code[b, 8 : 8 + y_blocks, :] = dot(table[b].astype(jnp.float32).astype(jnp.bfloat16), wide)
        code[b, 8 + y_blocks :, :] = jnp.full((8, columns), 2.0, jnp.float32)

    def codes_of(b, start, count):
        first = start // CELLS + 7
        return jnp.concatenate(
            [jnp.broadcast_to(code[b, pl.ds(first + k, 1), :], (CELLS, columns)) for k in range(count // CELLS)], axis=0)

    def physical(codes, z, start):
        return jnp.where(codes >= 1.5, field[z, pl.ds(start, codes.shape[0]), :], codes)

    def y_copies():
        return (
            (after, before, pltpu.make_async_remote_copy(
                src_ref=edges.at[1], dst_ref=field.at[:, pl.ds(0, PAD)],
                send_sem=y_send.at[1], recv_sem=y_recv.at[1], device_id={"gy": gy + 1})),
            (before, after, pltpu.make_async_remote_copy(
                src_ref=edges.at[0], dst_ref=field.at[:, pl.ds(PAD + rows, PAD)],
                send_sem=y_send.at[0], recv_sem=y_recv.at[0], device_id={"gy": gy - 1})),
        )

    def part_of(c):
        return pl.ds(pl.multiple_of(c * ROWS, ROWS), ROWS)

    def z_up(c):
        return above, below, pltpu.make_async_remote_copy(
            src_ref=smooth.at[pl.ds(planes, RADIUS), part_of(c)], dst_ref=smooth.at[pl.ds(0, RADIUS), part_of(c)],
            send_sem=z_send.at[0, c], recv_sem=z_recv.at[0, c], device_id={"gz": gz + 1})

    def z_down(c):
        return below, above, pltpu.make_async_remote_copy(
            src_ref=smooth.at[pl.ds(RADIUS, RADIUS), part_of(c)],
            dst_ref=smooth.at[pl.ds(RADIUS + planes, RADIUS), part_of(c)],
            send_sem=z_send.at[1, c], recv_sem=z_recv.at[1, c], device_id={"gz": gz - 1})

    def z_copies(c):
        return z_up(c), z_down(c)

    def span(g, late):
        last = n_x - 1
        if isinstance(g, int):
            return (free if g == last else 0, RADIUS) if late else (0 if g == last else RADIUS, free)
        return (jnp.where(g == last, free, 0), RADIUS) if late else (jnp.where(g == last, 0, RADIUS), free)

    def x_copy(g, c, late, target):
        z = pl.ds(*span(g, late))
        return pltpu.make_async_remote_copy(
            src_ref=layers.at[g, z, part_of(c)], dst_ref=lines.at[gx, z, part_of(c)],
            send_sem=send.at[c, g, late], recv_sem=recv.at[c, gx, late], device_id={"gx": target})

    def x_arrival(source, c, late):
        z = pl.ds(*span(gx, late))
        return pltpu.make_async_remote_copy(
            src_ref=layers.at[source, z, part_of(c)], dst_ref=lines.at[source, z, part_of(c)],
            send_sem=send.at[c, source, late], recv_sem=recv.at[c, source, late], device_id={"gx": source})

    def along_y(c, which):
        start = pl.multiple_of(c * ROWS, ROWS)
        scale = jnp.concatenate([inv_y[pl.ds(start, ROWS), :]] * (columns // 128), axis=1)
        window = ROWS + 2 * PAD
        for b in which:
            codes = codes_of(b, start, window)

            def plane(i, _):
                z = b * CELLS + i
                x = physical(codes, z, start)
                x2 = x + pltpu.roll(x, window - 1, 0)
                x4 = x2 + pltpu.roll(x2, window - 2, 0)
                x7 = x4 + (pltpu.roll(x2, window - 4, 0) + pltpu.roll(x, window - 6, 0))
                x2 = x7 + pltpu.roll(x7, 1, 0)
                x4 = x2 + pltpu.roll(x2, 2, 0)
                x7 = x4 + (pltpu.roll(x2, 4, 0) + pltpu.roll(x7, 6, 0))
                smooth[z + RADIUS, pl.ds(start, ROWS), :] = x7[PAD : PAD + ROWS] * scale
                return 0
            lax.fori_loop(0, CELLS, plane, 0, unroll=2)

    def along_z(g, c, first, count):
        def half(i, _):
            part = pl.ds(pl.multiple_of(c * ROWS + i * 8, 8), 8)
            base = g * group + first
            x = [smooth[base + k, part, :] for k in range(count + 2 * RADIUS)]
            for _ in range(2):
                x2 = [p + q for p, q in zip(x, x[1:])]
                x4 = [p + q for p, q in zip(x2, x2[2:])]
                x = [p + (q + r) for p, q, r in zip(x4, x2[4:], x[6:])]
            for k in range(count):
                x[k] = x[k] * jnp.concatenate([inv_z[base + k]] * (columns // 128), axis=1)

            @pl.when(g == gx)
            def _():
                for k in range(count):
                    lines[g, first + k, part, :] = x[k]

            @pl.when(g != gx)
            def _():
                for k in range(count):
                    layers[g, first + k, part, :] = x[k]
            return 0
        lax.fori_loop(0, ROWS // 8, half, 0)

    def start_when(copies):
        for sends, _, copy in copies:
            @pl.when(sends)
            def _():
                copy.start()

    def wait_recv_when(copies):
        for _, receives, copy in copies:
            @pl.when(receives)
            def _():
                copy.wait_recv()

    def wait_send_when(copies):
        for sends, _, copy in copies:
            @pl.when(sends)
            def _():
                copy.wait_send()

    def send_x(g, c, late):
        @pl.when(g != gx)
        def _():
            x_copy(g, c, late, g).start()

    def chunk(i):
        return lax.rem(i + 1, chunks)

    def early_planes(c):
        for g in (0, n_x - 1):
            along_z(g, c, *span(g, 0))
        for g in range(1, n_x - 1):
            along_z(g, c, 0, group)

    def send_early(c):
        for g in (0, n_x - 1):
            send_x(g, c, 0)
        for g in range(1, n_x - 1):
            send_x(g, c, 0)
            send_x(g, c, 1)

    def late(c):
        for g, arrival in ((0, z_up), (n_x - 1, z_down)):
            wait_recv_when([arrival(c)])
            along_z(g, c, *span(g, 1))
            send_x(g, c, 1)

    for b in range(blocks):
        load(0, b).wait()
    along_y(chunk(0), range(blocks))
    early_planes(chunk(0))
    expected = n_x - 1 + sum(t.astype(jnp.int32) for t in (below, above, before, after))
    pl.semaphore_wait(barrier, expected)
    start_when(z_copies(chunk(0)))
    send_early(chunk(0))
    for b in range(blocks):
        load(1, b).wait()

    def produce(i, _):
        @pl.when(i == chunks - 3)
        def _():
            wait_recv_when(y_copies())

        @pl.when(i < chunks - 1)
        def _():
            c = chunk(i + 1)
            along_y(c, outer)
            start_when(z_copies(c))
            along_y(c, inner)
            early_planes(c)
            send_early(c)

        @pl.when(i == 0)
        def _():
            for b in range(blocks):
                low, high = codes_of(b, PAD, PAD), codes_of(b, rows, PAD)

                def edge(k, _):
                    z = b * CELLS + k
                    edges[0, z] = physical(low, z, PAD)
                    edges[1, z] = physical(high, z, rows)
                    return 0
                lax.fori_loop(0, CELLS, edge, 0, unroll=4)
            start_when(y_copies())

        @pl.when(i >= LAG)
        def _():
            late(chunk(i - LAG))
        return 0

    lax.fori_loop(0, chunks + LAG, produce, 0)

    square = (columns, columns)
    near[...] = hat(iota(square, 0) - iota(square, 1)).astype(jnp.bfloat16)
    source = iota(square, 0)
    source = jnp.where(source < columns // 2, source - columns // 2, source + columns // 2)
    far[...] = hat(source - iota(square, 1)).astype(jnp.bfloat16)

    def wait_lines(c):
        for s in range(n_x):
            @pl.when(s != gx)
            def _():
                x_arrival(s, c, 0).wait_recv()
                x_arrival(s, c, 1).wait_recv()

    def consume(i, _):
        c = chunk(i)
        wait_lines(c)
        along_x(lines, part_of(c), near, far, filtered, projected, part_of(c))
        return 0

    lax.fori_loop(0, chunks - 1, consume, 0)

    def drain(c, _):
        wait_send_when(z_copies(c))
        for g in range(n_x):
            @pl.when(g != gx)
            def _():
                x_copy(g, c, 0, g).wait_send()
                x_copy(g, c, 1, g).wait_send()
        return 0

    lax.fori_loop(0, chunks, drain, 0)
    wait_send_when(y_copies())
    wait_lines(0)


def solution(mesh):
    sizes = tuple(mesh.shape[a] for a in ("gz", "gx", "gy"))
    n_x = sizes[1]

    def body(density, mask):
        planes, rows, columns = density.shape
        group, chunks = planes // n_x, rows // ROWS
        out = jax.ShapeDtypeStruct((group, rows, columns * n_x), jnp.float32)
        dma = pltpu.SemaphoreType.DMA
        vmem, hbm = pl.BlockSpec(memory_space=pltpu.VMEM), pl.BlockSpec(memory_space=pltpu.HBM)
        square = jax.ShapeDtypeStruct((columns, columns), jnp.bfloat16)
        lines = jax.ShapeDtypeStruct((n_x, group, rows, columns), jnp.float32)
        filtered, projected, lines, near, far = pl.pallas_call(
            functools.partial(kernel, sizes),
            out_shape=(out, out, lines, square, square),
            in_specs=[hbm] * 2,
            out_specs=[vmem] * 5,
            scratch_shapes=[
                pltpu.VMEM((planes, rows + 2 * PAD, columns), jnp.float32),
                pltpu.VMEM(mask.shape, jnp.int32),
                pltpu.VMEM((planes // CELLS, rows // CELLS + 16, columns), jnp.float32),
                pltpu.VMEM((2, planes, PAD, columns), jnp.float32),
                pltpu.VMEM((planes + 2 * RADIUS, rows, columns), jnp.float32),
                pltpu.VMEM((n_x, group, rows, columns), jnp.float32),
                pltpu.VMEM((rows, 128), jnp.float32),
                pltpu.VMEM((planes, 8, 128), jnp.float32),
                dma((3, planes // CELLS)),
                dma((chunks, n_x, 2)),
                dma((chunks, n_x, 2)),
                dma((2, chunks)),
                dma((2, chunks)),
                dma((2,)),
                dma((2,)),
            ],
            compiler_params=pltpu.CompilerParams(
                collective_id=0, has_side_effects=True, vmem_limit_bytes=22 * 2**20
            ),
        )(*(pltpu.with_memory_space_constraint(a, pltpu.HBM) for a in (density, mask)))
        return pl.pallas_call(
            finish,
            out_shape=(out, out),
            in_specs=[vmem] * 5,
            out_specs=[hbm] * 2,
            scratch_shapes=[
                pltpu.VMEM((group, ROWS, columns * n_x), jnp.float32),
                pltpu.VMEM((group, ROWS, columns * n_x), jnp.float32),
                dma((2, group + 1)),
            ],
            compiler_params=pltpu.CompilerParams(vmem_limit_bytes=8 * 2**20),
        )(lines, near, far, filtered, projected)

    return jax.shard_map(
        body,
        mesh=mesh,
        in_specs=(P("gz", "gy", "gx"), P("gz", "gy", "gx")),
        out_specs=(P(("gz", "gx"), "gy", None), P(("gz", "gx"), "gy", None)),
        check_vma=False,
    )
```

```python
import functools
import math

import jax
import jax.numpy as jnp
from jax import lax
from jax.experimental import pallas as pl
from jax.experimental.pallas import tpu as pltpu
from jax.sharding import PartitionSpec as P

RADIUS = 6
CELLS = 8
PAD = 8
ROWS = 16
LAG = 2

sharpness = 8.0
threshold = 0.5
top = math.tanh(sharpness * threshold)


def one_side(reach):
    return reach * (RADIUS + 1) - reach * (reach + 1) // 2


def inverse_count(position, length_all):
    reach_left = jnp.minimum(position, RADIUS)
    reach_right = jnp.minimum(length_all - 1 - position, RADIUS)
    return 1.0 / (RADIUS + 1 + one_side(reach_left) + one_side(reach_right)).astype(jnp.float32)


def iota(shape, dim):
    return lax.broadcasted_iota(jnp.int32, shape, dim)


def hat(distance):
    return jnp.maximum(RADIUS + 1 - jnp.abs(distance), 0).astype(jnp.float32)


def split(values):
    high = values.astype(jnp.bfloat16)
    return high, (values - high.astype(jnp.float32)).astype(jnp.bfloat16)


def dot(a, b):
    return jnp.dot(a, b, preferred_element_type=jnp.float32)


def along_x(lines, rows, near, far, filtered, projected, out_rows):
    n_x, planes, _, columns = lines.shape
    half = columns // 2
    parts = [split(lines[s, :, rows, :].reshape(planes * ROWS, columns)) for s in range(n_x)]
    for s in range(n_x):
        total = dot(parts[s][0], near[...]) + dot(parts[s][1], near[...])
        for j in range(2):
            if s == 0:
                total += dot(parts[1][j][:, :half], far[half:, :])
            elif s == n_x - 1:
                total += dot(parts[s - 1][j][:, half:], far[:half, :])
            else:
                total += dot(jnp.concatenate([parts[s - 1][j][:, half:], parts[s + 1][j][:, :half]], axis=1), far[...])
        total = total * inverse_count(s * columns + iota((1, columns), 1), n_x * columns)
        after_tanh = 0.5 + jnp.tanh(sharpness * total - sharpness * threshold) * (0.5 / top)
        filtered[:, out_rows, pl.ds(s * columns, columns)] = total.reshape(planes, ROWS, columns)
        projected[:, out_rows, pl.ds(s * columns, columns)] = after_tanh.reshape(planes, ROWS, columns)


def finish(lines, near, far, filtered, projected, filtered_out, projected_out, last_filtered, last_projected, sem):
    planes, rows, _ = filtered.shape
    rest = pl.ds(ROWS, rows - ROWS)
    copies = []
    for i, (source, target) in enumerate(((filtered, filtered_out), (projected, projected_out))):
        for z in range(planes):
            copies.append(pltpu.make_async_copy(source.at[z, rest], target.at[z, rest], sem.at[i]))
    for copy in copies:
        copy.start()
    first = pl.ds(0, ROWS)
    along_x(lines, first, near, far, last_filtered, last_projected, first)
    for i, (source, target) in enumerate(((last_filtered, filtered_out), (last_projected, projected_out))):
        pltpu.make_async_copy(source, target.at[:, first], sem.at[i]).start()
    for i, (source, target) in enumerate(((filtered, filtered_out), (projected, projected_out))):
        pltpu.make_async_copy(source, target, sem.at[i]).wait()


def kernel(sizes, density, mask, filtered, projected, lines, near, far, field, table, code, edges, smooth, layers,
           inv_y, inv_z, in_sem, send, recv, z_send, z_recv, y_send, y_recv):
    n_z, n_x, n_y = sizes
    planes, rows, columns = density.shape
    group = planes // n_x
    chunks = rows // ROWS
    blocks = planes // CELLS
    free = group - RADIUS
    gz, gx, gy = (lax.axis_index(a) for a in ("gz", "gx", "gy"))
    below, above = gz > 0, gz < n_z - 1
    before, after = gy > 0, gy < n_y - 1
    outer, inner = (0, blocks - 1), tuple(range(1, blocks - 1))

    head = 3 * ROWS
    load_mask = pltpu.make_async_copy(mask, table, in_sem.at[0])

    def load(part, b, count_b=1):
        start, count = ((0, head), (head, rows - head))[part > 1]
        z = pl.ds(b * CELLS, count_b * CELLS)
        return pltpu.make_async_copy(
            density.at[z, pl.ds(start, count)], field.at[z, pl.ds(PAD + start, count)], in_sem.at[1 + part])

    load_mask.start()
    for part, which in enumerate((outer, inner, range(blocks))):
        for b in which:
            load(part, b).start()

    barrier = pltpu.get_barrier_semaphore()
    for d in range(1, n_x):
        pl.semaphore_signal(barrier, inc=1, device_id={"gx": lax.rem(gx + d, n_x)})
    for there, axis, peer in (
        (below, "gz", gz - 1), (above, "gz", gz + 1), (before, "gy", gy - 1), (after, "gy", gy + 1)
    ):
        @pl.when(there)
        def _():
            pl.semaphore_signal(barrier, inc=1, device_id={axis: peer})

    inv_y[...] = inverse_count(gy * rows + iota(inv_y.shape, 0), n_y * rows)
    inv_z[...] = inverse_count(gz * planes + iota(inv_z.shape, 0), n_z * planes)

    @pl.when(jnp.logical_not(below))
    def _():
        smooth[0:RADIUS] = jnp.zeros((RADIUS, rows, columns), jnp.float32)

    @pl.when(jnp.logical_not(above))
    def _():
        smooth[RADIUS + planes :] = jnp.zeros((RADIUS, rows, columns), jnp.float32)

    @pl.when(jnp.logical_not(before))
    def _():
        field[:, 0:PAD, :] = jnp.zeros((planes, PAD, columns), jnp.float32)

    @pl.when(jnp.logical_not(after))
    def _():
        field[:, PAD + rows :, :] = jnp.zeros((planes, PAD, columns), jnp.float32)

    wide = jnp.where(iota((mask.shape[2], columns), 1) // CELLS == iota((mask.shape[2], columns), 0), 1.0, 0.0)
    wide = wide.astype(jnp.bfloat16)
    y_blocks = rows // CELLS
    load_mask.wait()
    for b in range(blocks):
        code[b, 0:8, :] = jnp.full((8, columns), 2.0, jnp.float32)
        code[b, 8 : 8 + y_blocks, :] = dot(table[b].astype(jnp.float32).astype(jnp.bfloat16), wide)
        code[b, 8 + y_blocks :, :] = jnp.full((8, columns), 2.0, jnp.float32)

    def codes_of(b, start, count):
        first = start // CELLS + 7
        return jnp.concatenate(
            [jnp.broadcast_to(code[b, pl.ds(first + k, 1), :], (CELLS, columns)) for k in range(count // CELLS)], axis=0)

    def physical(codes, z, start):
        return jnp.where(codes >= 1.5, field[z, pl.ds(start, codes.shape[0]), :], codes)

    def y_copies():
        return (
            (after, before, pltpu.make_async_remote_copy(
                src_ref=edges.at[1], dst_ref=field.at[:, pl.ds(0, PAD)],
                send_sem=y_send.at[1], recv_sem=y_recv.at[1], device_id={"gy": gy + 1})),
            (before, after, pltpu.make_async_remote_copy(
                src_ref=edges.at[0], dst_ref=field.at[:, pl.ds(PAD + rows, PAD)],
                send_sem=y_send.at[0], recv_sem=y_recv.at[0], device_id={"gy": gy - 1})),
        )

    def part_of(c):
        return pl.ds(pl.multiple_of(c * ROWS, ROWS), ROWS)

    def z_up(part):
        return above, below, pltpu.make_async_remote_copy(
            src_ref=smooth.at[pl.ds(planes, RADIUS), part[0]], dst_ref=smooth.at[pl.ds(0, RADIUS), part[0]],
            send_sem=z_send.at[0], recv_sem=z_recv.at[0, part[1]], device_id={"gz": gz + 1})

    def z_down(part):
        return below, above, pltpu.make_async_remote_copy(
            src_ref=smooth.at[pl.ds(RADIUS, RADIUS), part[0]],
            dst_ref=smooth.at[pl.ds(RADIUS + planes, RADIUS), part[0]],
            send_sem=z_send.at[1], recv_sem=z_recv.at[1, part[1]], device_id={"gz": gz - 1})

    def z_copies(c):
        part = (pl.ds(0, rows), 0) if c is None else (part_of(c), c)
        return z_up(part), z_down(part)

    def span(g, late):
        last = n_x - 1
        if isinstance(g, int):
            return (free if g == last else 0, RADIUS) if late else (0 if g == last else RADIUS, free)
        return (jnp.where(g == last, free, 0), RADIUS) if late else (jnp.where(g == last, 0, RADIUS), free)

    def x_copy(g, c, late, target):
        z = pl.ds(*span(g, late))
        return pltpu.make_async_remote_copy(
            src_ref=layers.at[g, z, part_of(c)], dst_ref=lines.at[gx, z, part_of(c)],
            send_sem=send.at[0], recv_sem=recv.at[c], device_id={"gx": target})

    def x_all(c):
        part = pl.ds(0, rows) if c is None else part_of(c)
        others = pl.ds(0, n_x - 1)
        return pltpu.make_async_remote_copy(
            src_ref=layers.at[others, :, part], dst_ref=lines.at[others, :, part], send_sem=send.at[0],
            recv_sem=recv.at[0 if c is None else c], device_id={"gx": lax.rem(gx + 1, n_x)})

    def along_y(c, which):
        start = pl.multiple_of(c * ROWS, ROWS)
        scale = jnp.concatenate([inv_y[pl.ds(start, ROWS), :]] * (columns // 128), axis=1)
        window = ROWS + 2 * PAD
        for b in which:
            codes = codes_of(b, start, window)

            def plane(i, _):
                z = b * CELLS + i
                x = physical(codes, z, start)
                x2 = x + pltpu.roll(x, window - 1, 0)
                x4 = x2 + pltpu.roll(x2, window - 2, 0)
                x7 = x4 + (pltpu.roll(x2, window - 4, 0) + pltpu.roll(x, window - 6, 0))
                x2 = x7 + pltpu.roll(x7, 1, 0)
                x4 = x2 + pltpu.roll(x2, 2, 0)
                x7 = x4 + (pltpu.roll(x2, 4, 0) + pltpu.roll(x7, 6, 0))
                smooth[z + RADIUS, pl.ds(start, ROWS), :] = x7[PAD : PAD + ROWS] * scale
                return 0
            lax.fori_loop(0, CELLS, plane, 0, unroll=2)

    def along_z(g, c, first, count):
        def half(i, _):
            part = pl.ds(pl.multiple_of(c * ROWS + i * 8, 8), 8)
            base = g * group + first
            x = [smooth[base + k, part, :] for k in range(count + 2 * RADIUS)]
            for _ in range(2):
                x2 = [p + q for p, q in zip(x, x[1:])]
                x4 = [p + q for p, q in zip(x2, x2[2:])]
                x = [p + (q + r) for p, q, r in zip(x4, x2[4:], x[6:])]
            for k in range(count):
                x[k] = x[k] * jnp.concatenate([inv_z[base + k]] * (columns // 128), axis=1)

            @pl.when(g == gx)
            def _():
                for k in range(count):
                    lines[g, first + k, part, :] = x[k]

            @pl.when(g != gx)
            def _():
                for k in range(count):
                    layers[g, first + k, part, :] = x[k]
            return 0
        lax.fori_loop(0, ROWS // 8, half, 0)

    def start_when(copies):
        for sends, _, copy in copies:
            @pl.when(sends)
            def _():
                copy.start()

    def wait_recv_when(copies):
        for _, receives, copy in copies:
            @pl.when(receives)
            def _():
                copy.wait_recv()

    def wait_send_when(copies):
        for sends, _, copy in copies:
            @pl.when(sends)
            def _():
                copy.wait_send()

    def send_x(g, c, late):
        @pl.when(g != gx)
        def _():
            x_copy(g, c, late, g).start()

    def chunk(i):
        return lax.rem(i + 1, chunks)

    def early_planes(c):
        for g in (0, n_x - 1):
            along_z(g, c, *span(g, 0))
        for g in range(1, n_x - 1):
            along_z(g, c, 0, group)

    def send_early(c):
        for g in (0, n_x - 1):
            send_x(g, c, 0)
        for g in range(1, n_x - 1):
            send_x(g, c, 0)
            send_x(g, c, 1)

    def late(c):
        for g, arrival in ((0, z_up), (n_x - 1, z_down)):
            wait_recv_when([arrival((part_of(c), c))])
            along_z(g, c, *span(g, 1))
            send_x(g, c, 1)

    load(0, 0, len(outer)).wait()
    along_y(chunk(0), outer)
    load(1, 0, len(inner)).wait()
    along_y(chunk(0), inner)
    early_planes(chunk(0))
    expected = n_x - 1 + sum(t.astype(jnp.int32) for t in (below, above, before, after))
    pl.semaphore_wait(barrier, expected)
    start_when(z_copies(chunk(0)))
    send_early(chunk(0))
    load(2, 0, blocks).wait()

    def produce(i, _):
        @pl.when(i == chunks - 3)
        def _():
            wait_recv_when(y_copies())

        @pl.when(i < chunks - 1)
        def _():
            c = chunk(i + 1)
            along_y(c, outer)
            start_when(z_copies(c))
            along_y(c, inner)
            early_planes(c)
            send_early(c)

        @pl.when(i == 0)
        def _():
            for b in range(blocks):
                low, high = codes_of(b, PAD, PAD), codes_of(b, rows, PAD)

                def edge(k, _):
                    z = b * CELLS + k
                    edges[0, z] = physical(low, z, PAD)
                    edges[1, z] = physical(high, z, rows)
                    return 0
                lax.fori_loop(0, CELLS, edge, 0, unroll=4)
            start_when(y_copies())

        @pl.when(i >= LAG)
        def _():
            late(chunk(i - LAG))
        return 0

    lax.fori_loop(0, chunks + LAG, produce, 0)

    square = (columns, columns)
    near[...] = hat(iota(square, 0) - iota(square, 1)).astype(jnp.bfloat16)
    source = iota(square, 0)
    source = jnp.where(source < columns // 2, source - columns // 2, source + columns // 2)
    far[...] = hat(source - iota(square, 1)).astype(jnp.bfloat16)

    def wait_lines(c):
        x_all(c).wait_recv()

    def consume(i, _):
        c = chunk(i)
        wait_lines(c)
        along_x(lines, part_of(c), near, far, filtered, projected, part_of(c))
        return 0

    lax.fori_loop(0, chunks - 1, consume, 0)

    wait_send_when(z_copies(None))
    x_all(None).wait_send()
    wait_send_when(y_copies())
    wait_lines(0)


def solution(mesh):
    sizes = tuple(mesh.shape[a] for a in ("gz", "gx", "gy"))
    n_x = sizes[1]

    def body(density, mask):
        planes, rows, columns = density.shape
        group, chunks = planes // n_x, rows // ROWS
        out = jax.ShapeDtypeStruct((group, rows, columns * n_x), jnp.float32)
        dma = pltpu.SemaphoreType.DMA
        vmem, hbm = pl.BlockSpec(memory_space=pltpu.VMEM), pl.BlockSpec(memory_space=pltpu.HBM)
        square = jax.ShapeDtypeStruct((columns, columns), jnp.bfloat16)
        lines = jax.ShapeDtypeStruct((n_x, group, rows, columns), jnp.float32)
        filtered, projected, lines, near, far = pl.pallas_call(
            functools.partial(kernel, sizes),
            out_shape=(out, out, lines, square, square),
            in_specs=[hbm] * 2,
            out_specs=[vmem] * 5,
            scratch_shapes=[
                pltpu.VMEM((planes, rows + 2 * PAD, columns), jnp.float32),
                pltpu.VMEM(mask.shape, jnp.int32),
                pltpu.VMEM((planes // CELLS, rows // CELLS + 16, columns), jnp.float32),
                pltpu.VMEM((2, planes, PAD, columns), jnp.float32),
                pltpu.VMEM((planes + 2 * RADIUS, rows, columns), jnp.float32),
                pltpu.VMEM((n_x, group, rows, columns), jnp.float32),
                pltpu.VMEM((rows, 128), jnp.float32),
                pltpu.VMEM((planes, 8, 128), jnp.float32),
                dma((4,)),
                dma((1,)),
                dma((chunks,)),
                dma((2,)),
                dma((2, chunks)),
                dma((2,)),
                dma((2,)),
            ],
            compiler_params=pltpu.CompilerParams(
                collective_id=0, has_side_effects=True, vmem_limit_bytes=22 * 2**20
            ),
        )(*(pltpu.with_memory_space_constraint(a, pltpu.HBM) for a in (density, mask)))
        return pl.pallas_call(
            finish,
            out_shape=(out, out),
            in_specs=[vmem] * 5,
            out_specs=[hbm] * 2,
            scratch_shapes=[
                pltpu.VMEM((group, ROWS, columns * n_x), jnp.float32),
                pltpu.VMEM((group, ROWS, columns * n_x), jnp.float32),
                dma((2,)),
            ],
            compiler_params=pltpu.CompilerParams(vmem_limit_bytes=8 * 2**20),
        )(lines, near, far, filtered, projected)

    return jax.shard_map(
        body,
        mesh=mesh,
        in_specs=(P("gz", "gy", "gx"), P("gz", "gy", "gx")),
        out_specs=(P(("gz", "gx"), "gy", None), P(("gz", "gx"), "gy", None)),
        check_vma=False,
    )
```

```python
import functools
import math

import jax
import jax.numpy as jnp
from jax import lax
from jax.experimental import pallas as pl
from jax.experimental.pallas import tpu as pltpu
from jax.sharding import PartitionSpec as P

RADIUS = 6
CELLS = 8
PAD = 8
ROWS = 16
LAG = 2

sharpness = 8.0
threshold = 0.5
top = math.tanh(sharpness * threshold)


def one_side(reach):
    return reach * (RADIUS + 1) - reach * (reach + 1) // 2


def inverse_count(position, length_all):
    reach_left = jnp.minimum(position, RADIUS)
    reach_right = jnp.minimum(length_all - 1 - position, RADIUS)
    return 1.0 / (RADIUS + 1 + one_side(reach_left) + one_side(reach_right)).astype(jnp.float32)


def iota(shape, dim):
    return lax.broadcasted_iota(jnp.int32, shape, dim)


def hat(distance):
    return jnp.maximum(RADIUS + 1 - jnp.abs(distance), 0).astype(jnp.float32)


def split(values):
    high = values.astype(jnp.bfloat16)
    return high, (values - high.astype(jnp.float32)).astype(jnp.bfloat16)


def dot(a, b):
    return jnp.dot(a, b, preferred_element_type=jnp.float32)


def along_x(lines, rows, near, far, filtered, projected, out_rows):
    n_x, planes, _, columns = lines.shape
    half = columns // 2
    parts = [split(lines[s, :, rows, :].reshape(planes * ROWS, columns)) for s in range(n_x)]
    for s in range(n_x):
        total = dot(parts[s][0], near[...]) + dot(parts[s][1], near[...])
        for j in range(2):
            if s == 0:
                total += dot(parts[1][j][:, :half], far[half:, :])
            elif s == n_x - 1:
                total += dot(parts[s - 1][j][:, half:], far[:half, :])
            else:
                total += dot(jnp.concatenate([parts[s - 1][j][:, half:], parts[s + 1][j][:, :half]], axis=1), far[...])
        total = total * inverse_count(s * columns + iota((1, columns), 1), n_x * columns)
        after_tanh = 0.5 + jnp.tanh(sharpness * total - sharpness * threshold) * (0.5 / top)
        filtered[:, out_rows, pl.ds(s * columns, columns)] = total.reshape(planes, ROWS, columns)
        projected[:, out_rows, pl.ds(s * columns, columns)] = after_tanh.reshape(planes, ROWS, columns)


def finish(lines, near, far, filtered, projected, filtered_out, projected_out, last_filtered, last_projected, sem):
    planes, rows, _ = filtered.shape
    rest = pl.ds(ROWS, rows - ROWS)
    copies = []
    for i, (source, target) in enumerate(((filtered, filtered_out), (projected, projected_out))):
        for z in range(planes):
            copies.append(pltpu.make_async_copy(source.at[z, rest], target.at[z, rest], sem.at[i]))
    for copy in copies:
        copy.start()
    first = pl.ds(0, ROWS)
    along_x(lines, first, near, far, last_filtered, last_projected, first)
    for i, (source, target) in enumerate(((last_filtered, filtered_out), (last_projected, projected_out))):
        pltpu.make_async_copy(source, target.at[:, first], sem.at[i]).start()
    for i, (source, target) in enumerate(((filtered, filtered_out), (projected, projected_out))):
        pltpu.make_async_copy(source, target, sem.at[i]).wait()


def kernel(sizes, density, mask, filtered, projected, lines, near, far, field, table, code, edges, smooth, layers,
           inv_y, inv_z, in_sem, send, recv, z_send, z_recv, y_send, y_recv, ready):
    n_z, n_x, n_y = sizes
    planes, rows, columns = density.shape
    group = planes // n_x
    chunks = rows // ROWS
    blocks = planes // CELLS
    free = group - RADIUS
    gz, gx, gy = (lax.axis_index(a) for a in ("gz", "gx", "gy"))
    below, above = gz > 0, gz < n_z - 1
    before, after = gy > 0, gy < n_y - 1
    outer, inner = (0, blocks - 1), tuple(range(1, blocks - 1))

    head = 3 * ROWS
    load_mask = pltpu.make_async_copy(mask, table, in_sem.at[0])

    def load(part, b, count_b=1):
        start, count = ((0, head), (head, rows - head))[part > 1]
        z = pl.ds(b * CELLS, count_b * CELLS)
        return pltpu.make_async_copy(
            density.at[z, pl.ds(start, count)], field.at[z, pl.ds(PAD + start, count)], in_sem.at[1 + part])

    load_mask.start()
    for part, which in enumerate((outer, inner, range(blocks))):
        for b in which:
            load(part, b).start()

    barrier = pltpu.get_barrier_semaphore()
    for d in range(1, n_x):
        pl.semaphore_signal(barrier, inc=1, device_id={"gx": lax.rem(gx + d, n_x)})
    for there, axis, peer in ((above, "gz", gz + 1), (after, "gy", gy + 1)):
        @pl.when(there)
        def _():
            pl.semaphore_signal(barrier, inc=1, device_id={axis: peer})

    inv_y[...] = inverse_count(gy * rows + iota(inv_y.shape, 0), n_y * rows)
    inv_z[...] = inverse_count(gz * planes + iota(inv_z.shape, 0), n_z * planes)

    @pl.when(jnp.logical_not(below))
    def _():
        smooth[0:RADIUS] = jnp.zeros((RADIUS, rows, columns), jnp.float32)

    @pl.when(jnp.logical_not(above))
    def _():
        smooth[RADIUS + planes :] = jnp.zeros((RADIUS, rows, columns), jnp.float32)

    @pl.when(jnp.logical_not(before))
    def _():
        field[:, 0:PAD, :] = jnp.zeros((planes, PAD, columns), jnp.float32)

    @pl.when(jnp.logical_not(after))
    def _():
        field[:, PAD + rows :, :] = jnp.zeros((planes, PAD, columns), jnp.float32)

    wide = jnp.where(iota((mask.shape[2], columns), 1) // CELLS == iota((mask.shape[2], columns), 0), 1.0, 0.0)
    wide = wide.astype(jnp.bfloat16)
    y_blocks = rows // CELLS
    with jax.named_scope("mask_wait"):
        load_mask.wait()
    for b in range(blocks):
        code[b, 0:8, :] = jnp.full((8, columns), 2.0, jnp.float32)
        code[b, 8 : 8 + y_blocks, :] = dot(table[b].astype(jnp.float32).astype(jnp.bfloat16), wide)
        code[b, 8 + y_blocks :, :] = jnp.full((8, columns), 2.0, jnp.float32)

    def codes_of(b, start, count):
        first = start // CELLS + 7
        return jnp.concatenate(
            [jnp.broadcast_to(code[b, pl.ds(first + k, 1), :], (CELLS, columns)) for k in range(count // CELLS)], axis=0)

    def physical(codes, z, start):
        return jnp.where(codes >= 1.5, field[z, pl.ds(start, codes.shape[0]), :], codes)

    def y_copies():
        return (
            (after, before, pltpu.make_async_remote_copy(
                src_ref=edges.at[1], dst_ref=field.at[:, pl.ds(0, PAD)],
                send_sem=y_send.at[1], recv_sem=y_recv.at[1], device_id={"gy": gy + 1})),
            (before, after, pltpu.make_async_remote_copy(
                src_ref=edges.at[0], dst_ref=field.at[:, pl.ds(PAD + rows, PAD)],
                send_sem=y_send.at[0], recv_sem=y_recv.at[0], device_id={"gy": gy - 1})),
        )

    def part_of(c):
        return pl.ds(pl.multiple_of(c * ROWS, ROWS), ROWS)

    def z_up(part):
        return above, below, pltpu.make_async_remote_copy(
            src_ref=smooth.at[pl.ds(planes, RADIUS), part[0]], dst_ref=smooth.at[pl.ds(0, RADIUS), part[0]],
            send_sem=z_send.at[0], recv_sem=z_recv.at[0, part[1]], device_id={"gz": gz + 1})

    def z_down(part):
        return below, above, pltpu.make_async_remote_copy(
            src_ref=smooth.at[pl.ds(RADIUS, RADIUS), part[0]],
            dst_ref=smooth.at[pl.ds(RADIUS + planes, RADIUS), part[0]],
            send_sem=z_send.at[1], recv_sem=z_recv.at[1, part[1]], device_id={"gz": gz - 1})

    def z_copies(c):
        part = (pl.ds(0, rows), 0) if c is None else (part_of(c), c)
        return z_up(part), z_down(part)

    def span(g, late):
        last = n_x - 1
        if isinstance(g, int):
            return (free if g == last else 0, RADIUS) if late else (0 if g == last else RADIUS, free)
        return (jnp.where(g == last, free, 0), RADIUS) if late else (jnp.where(g == last, 0, RADIUS), free)

    def x_copy(g, c, late, target):
        z = pl.ds(*span(g, late))
        return pltpu.make_async_remote_copy(
            src_ref=layers.at[g, z, part_of(c)], dst_ref=lines.at[gx, z, part_of(c)],
            send_sem=send.at[0], recv_sem=recv.at[c], device_id={"gx": target})

    def x_all(c):
        part = pl.ds(0, rows) if c is None else part_of(c)
        others = pl.ds(0, n_x - 1)
        return pltpu.make_async_remote_copy(
            src_ref=layers.at[others, :, part], dst_ref=lines.at[others, :, part], send_sem=send.at[0],
            recv_sem=recv.at[0 if c is None else c], device_id={"gx": lax.rem(gx + 1, n_x)})

    def along_y(c, which):
        start = pl.multiple_of(c * ROWS, ROWS)
        scale = jnp.concatenate([inv_y[pl.ds(start, ROWS), :]] * (columns // 128), axis=1)
        window = ROWS + 2 * PAD
        for b in which:
            codes = codes_of(b, start, window)

            def plane(i, _):
                z = b * CELLS + i
                x = physical(codes, z, start)
                x2 = x + pltpu.roll(x, window - 1, 0)
                x4 = x2 + pltpu.roll(x2, window - 2, 0)
                x7 = (x4 + pltpu.roll(x4 - x, window - 3, 0))[: PAD + ROWS]
                x2 = x7 + pltpu.roll(x7, 1, 0)
                x4 = x2 + pltpu.roll(x2, 2, 0)
                x7 = x4 + pltpu.roll(x4 - x7, 3, 0)
                smooth[z + RADIUS, pl.ds(start, ROWS), :] = x7[PAD:] * scale
                return 0
            lax.fori_loop(0, CELLS, plane, 0, unroll=8)

    def along_z(g, c, first, count):
        for i in range(ROWS // 8):
            part = pl.ds(pl.multiple_of(c * ROWS + i * 8, 8), 8)
            base = g * group + first
            x = [smooth[base + k, part, :] for k in range(count + 2 * RADIUS)]
            for _ in range(2):
                x2 = [p + q for p, q in zip(x, x[1:])]
                x4 = [p + q for p, q in zip(x2, x2[2:])]
                x = [p + (q + r) for p, q, r in zip(x4, x2[4:], x[6:])]
            for k in range(count):
                scale = jnp.concatenate([inv_z[base + k]] * (columns // 128), axis=1)
                layers[g, first + k, part, :] = x[k] * scale

    def start_when(copies):
        for sends, _, copy in copies:
            @pl.when(sends)
            def _():
                copy.start()

    def wait_recv_when(copies):
        for _, receives, copy in copies:
            @pl.when(receives)
            def _():
                copy.wait_recv()

    def wait_send_when(copies):
        for sends, _, copy in copies:
            @pl.when(sends)
            def _():
                copy.wait_send()

    def z_up_start(c):
        start_when([z_up((part_of(c), c))])

    def z_down_start(c):
        start_when([z_down((part_of(c), c))])

    def send_x(g, c, *which):
        @pl.when(g != gx)
        def _():
            for late in which:
                x_copy(g, c, late, g).start()

        @pl.when(g == gx)
        def _():
            for late in which:
                first, count = span(g, late)
                lines[g, pl.ds(first, count), part_of(c), :] = layers[g, pl.ds(first, count), part_of(c), :]

    def chunk(i):
        return lax.rem(i + 1, chunks)

    def early(c):
        for g in (0, n_x - 1):
            along_z(g, c, *span(g, 0))
            send_x(g, c, 0)
        for g in range(1, n_x - 1):
            along_z(g, c, 0, group)
            send_x(g, c, 0, 1)

    def late(c):
        for g, arrival in ((0, z_up), (n_x - 1, z_down)):
            with jax.named_scope("halo_wait"):
                wait_recv_when([arrival((part_of(c), c))])
            along_z(g, c, *span(g, 1))
            send_x(g, c, 1)

    with jax.named_scope("load_wait"):
        load(0, 0, len(outer)).wait()
    with jax.named_scope("first_y"):
        along_y(chunk(0), outer)
        load(1, 0, len(inner)).wait()
        along_y(chunk(0), inner)
    with jax.named_scope("barrier"):
        pl.semaphore_wait(barrier, n_x - 1 + below.astype(jnp.int32) + before.astype(jnp.int32))
    for there, axis, peer, i in ((below, "gz", gz - 1, 0), (before, "gy", gy - 1, 1)):
        @pl.when(there)
        def _():
            pl.semaphore_signal(ready.at[i], inc=1, device_id={axis: peer})
    z_down_start(chunk(0))
    with jax.named_scope("first_early"):
        early(chunk(0))
    load(2, 0, blocks).wait()

    def produce(i, _):
        @pl.when(i == chunks - 3)
        def _():
            wait_recv_when(y_copies())

        @pl.when(i < chunks - 1)
        def _():
            c = chunk(i + 1)
            along_y(c, outer)
            z_down_start(c)

            @pl.when(i > 0)
            def _():
                z_up_start(c)

            along_y(c, inner)
            early(c)

        @pl.when(i == 0)
        def _():
            for there, k in ((above, 0), (after, 1)):
                @pl.when(there)
                def _():
                    pl.semaphore_wait(ready.at[k], 1)
            z_up_start(chunk(0))
            z_up_start(chunk(1))
            for b in range(blocks):
                low, high = codes_of(b, PAD, PAD), codes_of(b, rows, PAD)

                def edge(k, _):
                    z = b * CELLS + k
                    edges[0, z] = physical(low, z, PAD)
                    edges[1, z] = physical(high, z, rows)
                    return 0
                lax.fori_loop(0, CELLS, edge, 0, unroll=4)
            start_when(y_copies())

        @pl.when(i >= LAG)
        def _():
            late(chunk(i - LAG))
        return 0

    lax.fori_loop(0, chunks + LAG, produce, 0)

    square = (columns, columns)
    near[...] = hat(iota(square, 0) - iota(square, 1)).astype(jnp.bfloat16)
    source = iota(square, 0)
    source = jnp.where(source < columns // 2, source - columns // 2, source + columns // 2)
    far[...] = hat(source - iota(square, 1)).astype(jnp.bfloat16)

    def wait_lines(c):
        x_all(c).wait_recv()

    def consume(i, _):
        c = chunk(i)
        with jax.named_scope("lines_wait"):
            wait_lines(c)
        with jax.named_scope("along_x"):
            along_x(lines, part_of(c), near, far, filtered, projected, part_of(c))
        return 0

    lax.fori_loop(0, chunks - 1, consume, 0)

    wait_send_when(z_copies(None))
    x_all(None).wait_send()
    wait_send_when(y_copies())
    with jax.named_scope("last_wait"):
        wait_lines(0)


def solution(mesh):
    sizes = tuple(mesh.shape[a] for a in ("gz", "gx", "gy"))
    n_x = sizes[1]

    def body(density, mask):
        planes, rows, columns = density.shape
        group, chunks = planes // n_x, rows // ROWS
        out = jax.ShapeDtypeStruct((group, rows, columns * n_x), jnp.float32)
        dma = pltpu.SemaphoreType.DMA
        vmem, hbm = pl.BlockSpec(memory_space=pltpu.VMEM), pl.BlockSpec(memory_space=pltpu.HBM)
        square = jax.ShapeDtypeStruct((columns, columns), jnp.bfloat16)
        lines = jax.ShapeDtypeStruct((n_x, group, rows, columns), jnp.float32)
        filtered, projected, lines, near, far = pl.pallas_call(
            functools.partial(kernel, sizes),
            out_shape=(out, out, lines, square, square),
            in_specs=[hbm] * 2,
            out_specs=[vmem] * 5,
            scratch_shapes=[
                pltpu.VMEM((planes, rows + 2 * PAD, columns), jnp.float32),
                pltpu.VMEM(mask.shape, jnp.int32),
                pltpu.VMEM((planes // CELLS, rows // CELLS + 16, columns), jnp.float32),
                pltpu.VMEM((2, planes, PAD, columns), jnp.float32),
                pltpu.VMEM((planes + 2 * RADIUS, rows, columns), jnp.float32),
                pltpu.VMEM((n_x, group, rows, columns), jnp.float32),
                pltpu.VMEM((rows, 128), jnp.float32),
                pltpu.VMEM((planes, 8, 128), jnp.float32),
                dma((4,)),
                dma((1,)),
                dma((chunks,)),
                dma((2,)),
                dma((2, chunks)),
                dma((2,)),
                dma((2,)),
                pltpu.SemaphoreType.REGULAR((2,)),
            ],
            compiler_params=pltpu.CompilerParams(
                collective_id=0, has_side_effects=True, vmem_limit_bytes=22 * 2**20
            ),
        )(*(pltpu.with_memory_space_constraint(a, pltpu.HBM) for a in (density, mask)))
        return pl.pallas_call(
            finish,
            out_shape=(out, out),
            in_specs=[vmem] * 5,
            out_specs=[hbm] * 2,
            scratch_shapes=[
                pltpu.VMEM((group, ROWS, columns * n_x), jnp.float32),
                pltpu.VMEM((group, ROWS, columns * n_x), jnp.float32),
                dma((2,)),
            ],
            compiler_params=pltpu.CompilerParams(vmem_limit_bytes=8 * 2**20),
        )(lines, near, far, filtered, projected)

    return jax.shard_map(
        body,
        mesh=mesh,
        in_specs=(P("gz", "gy", "gx"), P("gz", "gy", "gx")),
        out_specs=(P(("gz", "gx"), "gy", None), P(("gz", "gx"), "gy", None)),
        check_vma=False,
    )
```

```python
import functools
import math

import jax
import jax.numpy as jnp
from jax import lax
from jax.experimental import pallas as pl
from jax.experimental.pallas import tpu as pltpu
from jax.sharding import PartitionSpec as P

RADIUS = 6
CELLS = 8
PAD = 8
ROWS = 16
LAG = 2

sharpness = 8.0
threshold = 0.5
top = math.tanh(sharpness * threshold)


def one_side(reach):
    return reach * (RADIUS + 1) - reach * (reach + 1) // 2


def inverse_count(position, length_all):
    reach_left = jnp.minimum(position, RADIUS)
    reach_right = jnp.minimum(length_all - 1 - position, RADIUS)
    return 1.0 / (RADIUS + 1 + one_side(reach_left) + one_side(reach_right)).astype(jnp.float32)


def iota(shape, dim):
    return lax.broadcasted_iota(jnp.int32, shape, dim)


def hat(distance):
    return jnp.maximum(RADIUS + 1 - jnp.abs(distance), 0).astype(jnp.float32)


def split(values):
    high = values.astype(jnp.bfloat16)
    return high, (values - high.astype(jnp.float32)).astype(jnp.bfloat16)


def dot(a, b):
    return jnp.dot(a, b, preferred_element_type=jnp.float32)


def along_x(lines, rows, near, far, filtered, projected, out_rows):
    n_x, planes, _, columns = lines.shape
    half = columns // 2
    ends = jnp.tanh(jnp.full((8, columns), sharpness * threshold, jnp.float32))[:1]
    parts = [split(lines[s, :, rows, :].reshape(planes * ROWS, columns)) for s in range(n_x)]
    for s in range(n_x):
        total = dot(parts[s][0], near[...]) + dot(parts[s][1], near[...])
        for j in range(2):
            if s == 0:
                total += dot(parts[1][j][:, :half], far[half:, :])
            elif s == n_x - 1:
                total += dot(parts[s - 1][j][:, half:], far[:half, :])
            else:
                total += dot(jnp.concatenate([parts[s - 1][j][:, half:], parts[s + 1][j][:, :half]], axis=1), far[...])
        total = total * inverse_count(s * columns + iota((1, columns), 1), n_x * columns)
        after_tanh = (ends + jnp.tanh(sharpness * (total - threshold))) * (0.5 / top)
        filtered[:, out_rows, pl.ds(s * columns, columns)] = total.reshape(planes, ROWS, columns)
        projected[:, out_rows, pl.ds(s * columns, columns)] = after_tanh.reshape(planes, ROWS, columns)


def finish(lines, near, far, filtered, projected, filtered_out, projected_out, last_filtered, last_projected, sem):
    planes, rows, _ = filtered.shape
    rest = pl.ds(ROWS, rows - ROWS)
    copies = []
    for i, (source, target) in enumerate(((filtered, filtered_out), (projected, projected_out))):
        for z in range(planes):
            copies.append(pltpu.make_async_copy(source.at[z, rest], target.at[z, rest], sem.at[i]))
    for copy in copies:
        copy.start()
    first = pl.ds(0, ROWS)
    along_x(lines, first, near, far, last_filtered, last_projected, first)
    for i, (source, target) in enumerate(((last_filtered, filtered_out), (last_projected, projected_out))):
        pltpu.make_async_copy(source, target.at[:, first], sem.at[i]).start()
    for i, (source, target) in enumerate(((filtered, filtered_out), (projected, projected_out))):
        pltpu.make_async_copy(source, target, sem.at[i]).wait()


def kernel(sizes, density, mask, filtered, projected, lines, near, far, field, table, code, edges, smooth, layers,
           inv_y, inv_z, in_sem, send, recv, z_send, z_recv, y_send, y_recv, ready):
    n_z, n_x, n_y = sizes
    planes, rows, columns = density.shape
    group = planes // n_x
    chunks = rows // ROWS
    blocks = planes // CELLS
    free = group - RADIUS
    gz, gx, gy = (lax.axis_index(a) for a in ("gz", "gx", "gy"))
    below, above = gz > 0, gz < n_z - 1
    before, after = gy > 0, gy < n_y - 1
    outer, inner = (0, blocks - 1), tuple(range(1, blocks - 1))

    head = 3 * ROWS
    load_mask = pltpu.make_async_copy(mask, table, in_sem.at[0])

    def load(part, b, count_b=1):
        start, count = ((0, head), (head, rows - head))[part > 1]
        z = pl.ds(b * CELLS, count_b * CELLS)
        return pltpu.make_async_copy(
            density.at[z, pl.ds(start, count)], field.at[z, pl.ds(PAD + start, count)], in_sem.at[1 + part])

    load_mask.start()
    for part, which in enumerate((outer, inner, range(blocks))):
        for b in which:
            load(part, b).start()

    barrier = pltpu.get_barrier_semaphore()
    for d in range(1, n_x):
        pl.semaphore_signal(barrier, inc=1, device_id={"gx": lax.rem(gx + d, n_x)})
    for there, axis, peer in ((above, "gz", gz + 1), (after, "gy", gy + 1)):
        @pl.when(there)
        def _():
            pl.semaphore_signal(barrier, inc=1, device_id={axis: peer})

    inv_y[...] = inverse_count(gy * rows + iota(inv_y.shape, 0), n_y * rows)
    inv_z[...] = inverse_count(gz * planes + iota(inv_z.shape, 0), n_z * planes)

    @pl.when(jnp.logical_not(below))
    def _():
        smooth[0:RADIUS] = jnp.zeros((RADIUS, rows, columns), jnp.float32)

    @pl.when(jnp.logical_not(above))
    def _():
        smooth[RADIUS + planes :] = jnp.zeros((RADIUS, rows, columns), jnp.float32)

    @pl.when(jnp.logical_not(before))
    def _():
        field[:, 0:PAD, :] = jnp.zeros((planes, PAD, columns), jnp.float32)

    @pl.when(jnp.logical_not(after))
    def _():
        field[:, PAD + rows :, :] = jnp.zeros((planes, PAD, columns), jnp.float32)

    wide = jnp.where(iota((mask.shape[2], columns), 1) // CELLS == iota((mask.shape[2], columns), 0), 1.0, 0.0)
    wide = wide.astype(jnp.bfloat16)
    y_blocks = rows // CELLS
    with jax.named_scope("mask_wait"):
        load_mask.wait()
    for b in range(blocks):
        code[b, 0:8, :] = jnp.full((8, columns), 2.0, jnp.float32)
        code[b, 8 : 8 + y_blocks, :] = dot(table[b].astype(jnp.float32).astype(jnp.bfloat16), wide)
        code[b, 8 + y_blocks :, :] = jnp.full((8, columns), 2.0, jnp.float32)

    def codes_of(b, start, count):
        first = start // CELLS + 7
        return jnp.concatenate(
            [jnp.broadcast_to(code[b, pl.ds(first + k, 1), :], (CELLS, columns)) for k in range(count // CELLS)], axis=0)

    def physical(codes, z, start):
        return jnp.where(codes >= 1.5, field[z, pl.ds(start, codes.shape[0]), :], codes)

    def y_copies():
        return (
            (after, before, pltpu.make_async_remote_copy(
                src_ref=edges.at[1], dst_ref=field.at[:, pl.ds(0, PAD)],
                send_sem=y_send.at[1], recv_sem=y_recv.at[1], device_id={"gy": gy + 1})),
            (before, after, pltpu.make_async_remote_copy(
                src_ref=edges.at[0], dst_ref=field.at[:, pl.ds(PAD + rows, PAD)],
                send_sem=y_send.at[0], recv_sem=y_recv.at[0], device_id={"gy": gy - 1})),
        )

    def part_of(c):
        return pl.ds(pl.multiple_of(c * ROWS, ROWS), ROWS)

    def z_up(part):
        return above, below, pltpu.make_async_remote_copy(
            src_ref=smooth.at[pl.ds(planes, RADIUS), part[0]], dst_ref=smooth.at[pl.ds(0, RADIUS), part[0]],
            send_sem=z_send.at[0], recv_sem=z_recv.at[0, part[1]], device_id={"gz": gz + 1})

    def z_down(part):
        return below, above, pltpu.make_async_remote_copy(
            src_ref=smooth.at[pl.ds(RADIUS, RADIUS), part[0]],
            dst_ref=smooth.at[pl.ds(RADIUS + planes, RADIUS), part[0]],
            send_sem=z_send.at[1], recv_sem=z_recv.at[1, part[1]], device_id={"gz": gz - 1})

    def z_copies(c):
        part = (pl.ds(0, rows), 0) if c is None else (part_of(c), c)
        return z_up(part), z_down(part)

    def span(g, late):
        last = n_x - 1
        if isinstance(g, int):
            return (free if g == last else 0, RADIUS) if late else (0 if g == last else RADIUS, free)
        return (jnp.where(g == last, free, 0), RADIUS) if late else (jnp.where(g == last, 0, RADIUS), free)

    def x_copy(g, c, late, target):
        z = pl.ds(*span(g, late))
        return pltpu.make_async_remote_copy(
            src_ref=layers.at[g, z, part_of(c)], dst_ref=lines.at[gx, z, part_of(c)],
            send_sem=send.at[0], recv_sem=recv.at[c], device_id={"gx": target})

    def x_all(c):
        part = pl.ds(0, rows) if c is None else part_of(c)
        others = pl.ds(0, n_x - 1)
        return pltpu.make_async_remote_copy(
            src_ref=layers.at[others, :, part], dst_ref=lines.at[others, :, part], send_sem=send.at[0],
            recv_sem=recv.at[0 if c is None else c], device_id={"gx": lax.rem(gx + 1, n_x)})

    def along_y(c, which):
        start = pl.multiple_of(c * ROWS, ROWS)
        scale = jnp.concatenate([inv_y[pl.ds(start, ROWS), :]] * (columns // 128), axis=1)
        window = ROWS + 2 * PAD
        for b in which:
            codes = codes_of(b, start, window)

            def plane(i, _):
                z = b * CELLS + i
                x = physical(codes, z, start)
                x2 = x + pltpu.roll(x, window - 1, 0)
                x4 = x2 + pltpu.roll(x2, window - 2, 0)
                x7 = (x4 + pltpu.roll(x4 - x, window - 3, 0))[: PAD + ROWS]
                x2 = x7 + pltpu.roll(x7, 1, 0)
                x4 = x2 + pltpu.roll(x2, 2, 0)
                x7 = x4 + pltpu.roll(x4 - x7, 3, 0)
                smooth[z + RADIUS, pl.ds(start, ROWS), :] = x7[PAD:] * scale
                return 0
            lax.fori_loop(0, CELLS, plane, 0, unroll=8)

    def along_z(g, c, first, count):
        for i in range(ROWS // 8):
            part = pl.ds(pl.multiple_of(c * ROWS + i * 8, 8), 8)
            base = g * group + first
            x = [smooth[base + k, part, :] for k in range(count + 2 * RADIUS)]
            for _ in range(2):
                x2 = [p + q for p, q in zip(x, x[1:])]
                x4 = [p + q for p, q in zip(x2, x2[2:])]
                x = [p + (q + r) for p, q, r in zip(x4, x2[4:], x[6:])]
            for k in range(count):
                scale = jnp.concatenate([inv_z[base + k]] * (columns // 128), axis=1)
                layers[g, first + k, part, :] = x[k] * scale

    def start_when(copies):
        for sends, _, copy in copies:
            @pl.when(sends)
            def _():
                copy.start()

    def wait_recv_when(copies):
        for _, receives, copy in copies:
            @pl.when(receives)
            def _():
                copy.wait_recv()

    def wait_send_when(copies):
        for sends, _, copy in copies:
            @pl.when(sends)
            def _():
                copy.wait_send()

    def z_up_start(c):
        start_when([z_up((part_of(c), c))])

    def z_down_start(c):
        start_when([z_down((part_of(c), c))])

    def send_x(g, c, *which):
        @pl.when(g != gx)
        def _():
            for late in which:
                x_copy(g, c, late, g).start()

        @pl.when(g == gx)
        def _():
            for late in which:
                first, count = span(g, late)
                lines[g, pl.ds(first, count), part_of(c), :] = layers[g, pl.ds(first, count), part_of(c), :]

    def chunk(i):
        return lax.rem(i + 1, chunks)

    def early(c):
        for g in (0, n_x - 1):
            along_z(g, c, *span(g, 0))
            send_x(g, c, 0)
        for g in range(1, n_x - 1):
            along_z(g, c, 0, group)
            send_x(g, c, 0, 1)

    def late(c):
        for g, arrival in ((0, z_up), (n_x - 1, z_down)):
            with jax.named_scope("halo_wait"):
                wait_recv_when([arrival((part_of(c), c))])
            along_z(g, c, *span(g, 1))
            send_x(g, c, 1)

    with jax.named_scope("load_wait"):
        load(0, 0, len(outer)).wait()
    with jax.named_scope("first_y"):
        along_y(chunk(0), outer)
        load(1, 0, len(inner)).wait()
        along_y(chunk(0), inner)
    with jax.named_scope("barrier"):
        pl.semaphore_wait(barrier, n_x - 1 + below.astype(jnp.int32) + before.astype(jnp.int32))
    for there, axis, peer, i in ((below, "gz", gz - 1, 0), (before, "gy", gy - 1, 1)):
        @pl.when(there)
        def _():
            pl.semaphore_signal(ready.at[i], inc=1, device_id={axis: peer})
    z_down_start(chunk(0))
    with jax.named_scope("first_early"):
        early(chunk(0))
    load(2, 0, blocks).wait()

    def produce(i, _):
        @pl.when(i == chunks - 3)
        def _():
            wait_recv_when(y_copies())

        @pl.when(i < chunks - 1)
        def _():
            c = chunk(i + 1)
            along_y(c, outer)
            z_down_start(c)

            @pl.when(i > 0)
            def _():
                z_up_start(c)

            along_y(c, inner)
            early(c)

        @pl.when(i == 0)
        def _():
            for there, k in ((above, 0), (after, 1)):
                @pl.when(there)
                def _():
                    pl.semaphore_wait(ready.at[k], 1)
            z_up_start(chunk(0))
            z_up_start(chunk(1))
            for b in range(blocks):
                low, high = codes_of(b, PAD, PAD), codes_of(b, rows, PAD)

                def edge(k, _):
                    z = b * CELLS + k
                    edges[0, z] = physical(low, z, PAD)
                    edges[1, z] = physical(high, z, rows)
                    return 0
                lax.fori_loop(0, CELLS, edge, 0, unroll=4)
            start_when(y_copies())

        @pl.when(i >= LAG)
        def _():
            late(chunk(i - LAG))
        return 0

    lax.fori_loop(0, chunks + LAG, produce, 0)

    square = (columns, columns)
    near[...] = hat(iota(square, 0) - iota(square, 1)).astype(jnp.bfloat16)
    source = iota(square, 0)
    source = jnp.where(source < columns // 2, source - columns // 2, source + columns // 2)
    far[...] = hat(source - iota(square, 1)).astype(jnp.bfloat16)

    def wait_lines(c):
        x_all(c).wait_recv()

    def consume(i, _):
        c = chunk(i)
        with jax.named_scope("lines_wait"):
            wait_lines(c)
        with jax.named_scope("along_x"):
            along_x(lines, part_of(c), near, far, filtered, projected, part_of(c))
        return 0

    lax.fori_loop(0, chunks - 1, consume, 0)

    wait_send_when(z_copies(None))
    x_all(None).wait_send()
    wait_send_when(y_copies())
    with jax.named_scope("last_wait"):
        wait_lines(0)


def solution(mesh):
    sizes = tuple(mesh.shape[a] for a in ("gz", "gx", "gy"))
    n_x = sizes[1]

    def body(density, mask):
        planes, rows, columns = density.shape
        group, chunks = planes // n_x, rows // ROWS
        out = jax.ShapeDtypeStruct((group, rows, columns * n_x), jnp.float32)
        dma = pltpu.SemaphoreType.DMA
        vmem, hbm = pl.BlockSpec(memory_space=pltpu.VMEM), pl.BlockSpec(memory_space=pltpu.HBM)
        square = jax.ShapeDtypeStruct((columns, columns), jnp.bfloat16)
        lines = jax.ShapeDtypeStruct((n_x, group, rows, columns), jnp.float32)
        filtered, projected, lines, near, far = pl.pallas_call(
            functools.partial(kernel, sizes),
            out_shape=(out, out, lines, square, square),
            in_specs=[hbm] * 2,
            out_specs=[vmem] * 5,
            scratch_shapes=[
                pltpu.VMEM((planes, rows + 2 * PAD, columns), jnp.float32),
                pltpu.VMEM(mask.shape, jnp.int32),
                pltpu.VMEM((planes // CELLS, rows // CELLS + 16, columns), jnp.float32),
                pltpu.VMEM((2, planes, PAD, columns), jnp.float32),
                pltpu.VMEM((planes + 2 * RADIUS, rows, columns), jnp.float32),
                pltpu.VMEM((n_x, group, rows, columns), jnp.float32),
                pltpu.VMEM((rows, 128), jnp.float32),
                pltpu.VMEM((planes, 8, 128), jnp.float32),
                dma((4,)),
                dma((1,)),
                dma((chunks,)),
                dma((2,)),
                dma((2, chunks)),
                dma((2,)),
                dma((2,)),
                pltpu.SemaphoreType.REGULAR((2,)),
            ],
            compiler_params=pltpu.CompilerParams(
                collective_id=0, has_side_effects=True, vmem_limit_bytes=22 * 2**20
            ),
        )(*(pltpu.with_memory_space_constraint(a, pltpu.HBM) for a in (density, mask)))
        return pl.pallas_call(
            finish,
            out_shape=(out, out),
            in_specs=[vmem] * 5,
            out_specs=[hbm] * 2,
            scratch_shapes=[
                pltpu.VMEM((group, ROWS, columns * n_x), jnp.float32),
                pltpu.VMEM((group, ROWS, columns * n_x), jnp.float32),
                dma((2,)),
            ],
            compiler_params=pltpu.CompilerParams(vmem_limit_bytes=8 * 2**20),
        )(lines, near, far, filtered, projected)

    return jax.shard_map(
        body,
        mesh=mesh,
        in_specs=(P("gz", "gy", "gx"), P("gz", "gy", "gx")),
        out_specs=(P(("gz", "gx"), "gy", None), P(("gz", "gx"), "gy", None)),
        check_vma=False,
    )
```

```python
import functools
import math

import jax
import jax.numpy as jnp
from jax import lax
from jax.experimental import pallas as pl
from jax.experimental.pallas import tpu as pltpu
from jax.sharding import PartitionSpec as P

RADIUS = 6
CELLS = 8
PAD = 8
ROWS = 16
LAG = 2

sharpness = 8.0
threshold = 0.5
top = math.tanh(sharpness * threshold)


def one_side(reach):
    return reach * (RADIUS + 1) - reach * (reach + 1) // 2


def inverse_count(position, length_all):
    reach_left = jnp.minimum(position, RADIUS)
    reach_right = jnp.minimum(length_all - 1 - position, RADIUS)
    return 1.0 / (RADIUS + 1 + one_side(reach_left) + one_side(reach_right)).astype(jnp.float32)


def iota(shape, dim):
    return lax.broadcasted_iota(jnp.int32, shape, dim)


def hat(distance):
    return jnp.maximum(RADIUS + 1 - jnp.abs(distance), 0).astype(jnp.float32)


def split(values):
    high = values.astype(jnp.bfloat16)
    return high, (values - high.astype(jnp.float32)).astype(jnp.bfloat16)


def dot(a, b):
    return jnp.dot(a, b, preferred_element_type=jnp.float32)


def along_x(lines, rows, near, far, filtered, projected, out_rows):
    n_x, planes, _, columns = lines.shape
    half = columns // 2
    ends = jnp.tanh(jnp.full((8, columns), sharpness * threshold, jnp.float32))[:1]
    parts = [split(lines[s, :, rows, :].reshape(planes * ROWS, columns)) for s in range(n_x)]
    for s in range(n_x):
        total = dot(parts[s][0], near[...]) + dot(parts[s][1], near[...])
        for j in range(2):
            if s == 0:
                total += dot(parts[1][j][:, :half], far[half:, :])
            elif s == n_x - 1:
                total += dot(parts[s - 1][j][:, half:], far[:half, :])
            else:
                total += dot(jnp.concatenate([parts[s - 1][j][:, half:], parts[s + 1][j][:, :half]], axis=1), far[...])
        total = total * inverse_count(s * columns + iota((1, columns), 1), n_x * columns)
        after_tanh = (ends + jnp.tanh(sharpness * (total - threshold))) * (0.5 / top)
        filtered[:, out_rows, pl.ds(s * columns, columns)] = total.reshape(planes, ROWS, columns)
        projected[:, out_rows, pl.ds(s * columns, columns)] = after_tanh.reshape(planes, ROWS, columns)


def finish(lines, near, far, filtered, projected, filtered_out, projected_out, last_filtered, last_projected, sem):
    planes, rows, _ = filtered.shape
    rest = pl.ds(ROWS, rows - ROWS)
    copies = []
    for i, (source, target) in enumerate(((filtered, filtered_out), (projected, projected_out))):
        for z in range(planes):
            copies.append(pltpu.make_async_copy(source.at[z, rest], target.at[z, rest], sem.at[i]))
    for copy in copies:
        copy.start()
    first = pl.ds(0, ROWS)
    along_x(lines, first, near, far, last_filtered, last_projected, first)
    for i, (source, target) in enumerate(((last_filtered, filtered_out), (last_projected, projected_out))):
        pltpu.make_async_copy(source, target.at[:, first], sem.at[i]).start()
    for i, (source, target) in enumerate(((filtered, filtered_out), (projected, projected_out))):
        pltpu.make_async_copy(source, target, sem.at[i]).wait()


def kernel(sizes, density, mask, filtered, projected, lines, near, far, field, table, code, edges, smooth, layers,
           inv_y, inv_z, in_sem, send, recv, z_send, z_recv, y_send, y_recv, ready):
    n_z, n_x, n_y = sizes
    planes, rows, columns = density.shape
    group = planes // n_x
    chunks = rows // ROWS
    blocks = planes // CELLS
    free = group - RADIUS
    gz, gx, gy = (lax.axis_index(a) for a in ("gz", "gx", "gy"))
    below, above = gz > 0, gz < n_z - 1
    before, after = gy > 0, gy < n_y - 1
    outer, inner = (0, blocks - 1), tuple(range(1, blocks - 1))

    first, head = ROWS - PAD, ROWS + 2 * PAD
    load_mask = pltpu.make_async_copy(mask, table, in_sem.at[0])

    def load(part, b, count_b=1):
        start, count = ((first, head), (first, head), (0, first), (first + head, rows - first - head))[part]
        z = pl.ds(b * CELLS, count_b * CELLS)
        return pltpu.make_async_copy(
            density.at[z, pl.ds(start, count)], field.at[z, pl.ds(PAD + start, count)], in_sem.at[1 + part])

    load_mask.start()
    for part, which in enumerate((outer, inner)):
        for b in which:
            load(part, b).start()

    barrier = pltpu.get_barrier_semaphore()
    for d in range(1, n_x):
        pl.semaphore_signal(barrier, inc=1, device_id={"gx": lax.rem(gx + d, n_x)})
    for there, axis, peer in ((above, "gz", gz + 1), (after, "gy", gy + 1)):
        @pl.when(there)
        def _():
            pl.semaphore_signal(barrier, inc=1, device_id={axis: peer})

    for part in (2, 3):
        for b in range(blocks):
            load(part, b).start()

    inv_y[...] = inverse_count(gy * rows + iota(inv_y.shape, 0), n_y * rows)
    inv_z[...] = inverse_count(gz * planes + iota(inv_z.shape, 0), n_z * planes)

    @pl.when(jnp.logical_not(below))
    def _():
        smooth[0:RADIUS] = jnp.zeros((RADIUS, rows, columns), jnp.float32)

    @pl.when(jnp.logical_not(above))
    def _():
        smooth[RADIUS + planes :] = jnp.zeros((RADIUS, rows, columns), jnp.float32)

    @pl.when(jnp.logical_not(before))
    def _():
        field[:, 0:PAD, :] = jnp.zeros((planes, PAD, columns), jnp.float32)

    @pl.when(jnp.logical_not(after))
    def _():
        field[:, PAD + rows :, :] = jnp.zeros((planes, PAD, columns), jnp.float32)

    wide = jnp.where(iota((mask.shape[2], columns), 1) // CELLS == iota((mask.shape[2], columns), 0), 1.0, 0.0)
    wide = wide.astype(jnp.bfloat16)
    y_blocks = rows // CELLS
    with jax.named_scope("mask_wait"):
        load_mask.wait()
    for b in range(blocks):
        code[b, 0:8, :] = jnp.full((8, columns), 2.0, jnp.float32)
        code[b, 8 : 8 + y_blocks, :] = dot(table[b].astype(jnp.float32).astype(jnp.bfloat16), wide)
        code[b, 8 + y_blocks :, :] = jnp.full((8, columns), 2.0, jnp.float32)

    def codes_of(b, start, count):
        first = start // CELLS + 7
        return jnp.concatenate(
            [jnp.broadcast_to(code[b, pl.ds(first + k, 1), :], (CELLS, columns)) for k in range(count // CELLS)], axis=0)

    def physical(codes, z, start):
        return jnp.where(codes >= 1.5, field[z, pl.ds(start, codes.shape[0]), :], codes)

    def y_copies():
        return (
            (after, before, pltpu.make_async_remote_copy(
                src_ref=edges.at[1], dst_ref=field.at[:, pl.ds(0, PAD)],
                send_sem=y_send.at[1], recv_sem=y_recv.at[1], device_id={"gy": gy + 1})),
            (before, after, pltpu.make_async_remote_copy(
                src_ref=edges.at[0], dst_ref=field.at[:, pl.ds(PAD + rows, PAD)],
                send_sem=y_send.at[0], recv_sem=y_recv.at[0], device_id={"gy": gy - 1})),
        )

    def part_of(c):
        return pl.ds(pl.multiple_of(c * ROWS, ROWS), ROWS)

    def z_up(part):
        return above, below, pltpu.make_async_remote_copy(
            src_ref=smooth.at[pl.ds(planes, RADIUS), part[0]], dst_ref=smooth.at[pl.ds(0, RADIUS), part[0]],
            send_sem=z_send.at[0], recv_sem=z_recv.at[0, part[1]], device_id={"gz": gz + 1})

    def z_down(part):
        return below, above, pltpu.make_async_remote_copy(
            src_ref=smooth.at[pl.ds(RADIUS, RADIUS), part[0]],
            dst_ref=smooth.at[pl.ds(RADIUS + planes, RADIUS), part[0]],
            send_sem=z_send.at[1], recv_sem=z_recv.at[1, part[1]], device_id={"gz": gz - 1})

    def z_copies(c):
        part = (pl.ds(0, rows), 0) if c is None else (part_of(c), c)
        return z_up(part), z_down(part)

    def span(g, late):
        last = n_x - 1
        if isinstance(g, int):
            return (free if g == last else 0, RADIUS) if late else (0 if g == last else RADIUS, free)
        return (jnp.where(g == last, free, 0), RADIUS) if late else (jnp.where(g == last, 0, RADIUS), free)

    def x_copy(g, c, late, target):
        z = pl.ds(*span(g, late))
        return pltpu.make_async_remote_copy(
            src_ref=layers.at[g, z, part_of(c)], dst_ref=lines.at[gx, z, part_of(c)],
            send_sem=send.at[0], recv_sem=recv.at[c], device_id={"gx": target})

    def x_all(c):
        part = pl.ds(0, rows) if c is None else part_of(c)
        others = pl.ds(0, n_x - 1)
        return pltpu.make_async_remote_copy(
            src_ref=layers.at[others, :, part], dst_ref=lines.at[others, :, part], send_sem=send.at[0],
            recv_sem=recv.at[0 if c is None else c], device_id={"gx": lax.rem(gx + 1, n_x)})

    def along_y(c, which):
        start = pl.multiple_of(c * ROWS, ROWS)
        scale = jnp.concatenate([inv_y[pl.ds(start, ROWS), :]] * (columns // 128), axis=1)
        window = ROWS + 2 * PAD
        for b in which:
            codes = codes_of(b, start, window)

            def plane(i, _):
                z = b * CELLS + i
                x = physical(codes, z, start)
                x2 = x + pltpu.roll(x, window - 1, 0)
                x4 = x2 + pltpu.roll(x2, window - 2, 0)
                x7 = (x4 + pltpu.roll(x4 - x, window - 3, 0))[: PAD + ROWS]
                x2 = x7 + pltpu.roll(x7, 1, 0)
                x4 = x2 + pltpu.roll(x2, 2, 0)
                x7 = x4 + pltpu.roll(x4 - x7, 3, 0)
                smooth[z + RADIUS, pl.ds(start, ROWS), :] = x7[PAD:] * scale
                return 0
            lax.fori_loop(0, CELLS, plane, 0, unroll=8)

    def along_z(g, c, first, count):
        for i in range(ROWS // 8):
            part = pl.ds(pl.multiple_of(c * ROWS + i * 8, 8), 8)
            base = g * group + first
            x = [smooth[base + k, part, :] for k in range(count + 2 * RADIUS)]
            for _ in range(2):
                x2 = [p + q for p, q in zip(x, x[1:])]
                x4 = [p + q for p, q in zip(x2, x2[2:])]
                x = [p + (q + r) for p, q, r in zip(x4, x2[4:], x[6:])]
            for k in range(count):
                scale = jnp.concatenate([inv_z[base + k]] * (columns // 128), axis=1)
                layers[g, first + k, part, :] = x[k] * scale

    def start_when(copies):
        for sends, _, copy in copies:
            @pl.when(sends)
            def _():
                copy.start()

    def wait_recv_when(copies):
        for _, receives, copy in copies:
            @pl.when(receives)
            def _():
                copy.wait_recv()

    def wait_send_when(copies):
        for sends, _, copy in copies:
            @pl.when(sends)
            def _():
                copy.wait_send()

    def z_up_start(c):
        start_when([z_up((part_of(c), c))])

    def z_down_start(c):
        start_when([z_down((part_of(c), c))])

    def send_x(g, c, *which):
        @pl.when(g != gx)
        def _():
            for late in which:
                x_copy(g, c, late, g).start()

        @pl.when(g == gx)
        def _():
            for late in which:
                first, count = span(g, late)
                lines[g, pl.ds(first, count), part_of(c), :] = layers[g, pl.ds(first, count), part_of(c), :]

    def chunk(i):
        return lax.rem(i + 1, chunks)

    def early(c):
        for g in (0, n_x - 1):
            along_z(g, c, *span(g, 0))
            send_x(g, c, 0)
        for g in range(1, n_x - 1):
            along_z(g, c, 0, group)
            send_x(g, c, 0, 1)

    def late(c):
        for g, arrival in ((0, z_up), (n_x - 1, z_down)):
            with jax.named_scope("halo_wait"):
                wait_recv_when([arrival((part_of(c), c))])
            along_z(g, c, *span(g, 1))
            send_x(g, c, 1)

    with jax.named_scope("load_wait"):
        load(0, 0, len(outer)).wait()
    with jax.named_scope("first_y"):
        along_y(chunk(0), outer)
        load(1, 0, len(inner)).wait()
        along_y(chunk(0), inner)
    with jax.named_scope("barrier"):
        pl.semaphore_wait(barrier, n_x - 1 + below.astype(jnp.int32) + before.astype(jnp.int32))
    for there, axis, peer, i in ((below, "gz", gz - 1, 0), (before, "gy", gy - 1, 1)):
        @pl.when(there)
        def _():
            pl.semaphore_signal(ready.at[i], inc=1, device_id={axis: peer})
    z_down_start(chunk(0))
    with jax.named_scope("first_early"):
        early(chunk(0))
    load(2, 0, blocks).wait()
    load(3, 0, blocks).wait()

    def produce(i, _):
        @pl.when(i == chunks - 3)
        def _():
            wait_recv_when(y_copies())

        @pl.when(i < chunks - 1)
        def _():
            c = chunk(i + 1)
            along_y(c, outer)
            z_down_start(c)

            @pl.when(i > 0)
            def _():
                z_up_start(c)

            along_y(c, inner)
            early(c)

        @pl.when(i == 0)
        def _():
            for there, k in ((above, 0), (after, 1)):
                @pl.when(there)
                def _():
                    pl.semaphore_wait(ready.at[k], 1)
            z_up_start(chunk(0))
            z_up_start(chunk(1))
            for b in range(blocks):
                low, high = codes_of(b, PAD, PAD), codes_of(b, rows, PAD)

                def edge(k, _):
                    z = b * CELLS + k
                    edges[0, z] = physical(low, z, PAD)
                    edges[1, z] = physical(high, z, rows)
                    return 0
                lax.fori_loop(0, CELLS, edge, 0, unroll=4)
            start_when(y_copies())

        @pl.when(i >= LAG)
        def _():
            late(chunk(i - LAG))
        return 0

    lax.fori_loop(0, chunks + LAG, produce, 0)

    square = (columns, columns)
    near[...] = hat(iota(square, 0) - iota(square, 1)).astype(jnp.bfloat16)
    source = iota(square, 0)
    source = jnp.where(source < columns // 2, source - columns // 2, source + columns // 2)
    far[...] = hat(source - iota(square, 1)).astype(jnp.bfloat16)

    def wait_lines(c):
        x_all(c).wait_recv()

    def consume(i, _):
        c = chunk(i)
        with jax.named_scope("lines_wait"):
            wait_lines(c)
        with jax.named_scope("along_x"):
            along_x(lines, part_of(c), near, far, filtered, projected, part_of(c))
        return 0

    lax.fori_loop(0, chunks - 1, consume, 0)

    wait_send_when(z_copies(None))
    x_all(None).wait_send()
    wait_send_when(y_copies())
    with jax.named_scope("last_wait"):
        wait_lines(0)


def solution(mesh):
    sizes = tuple(mesh.shape[a] for a in ("gz", "gx", "gy"))
    n_x = sizes[1]

    def body(density, mask):
        planes, rows, columns = density.shape
        group, chunks = planes // n_x, rows // ROWS
        out = jax.ShapeDtypeStruct((group, rows, columns * n_x), jnp.float32)
        dma = pltpu.SemaphoreType.DMA
        vmem, hbm = pl.BlockSpec(memory_space=pltpu.VMEM), pl.BlockSpec(memory_space=pltpu.HBM)
        square = jax.ShapeDtypeStruct((columns, columns), jnp.bfloat16)
        lines = jax.ShapeDtypeStruct((n_x, group, rows, columns), jnp.float32)
        filtered, projected, lines, near, far = pl.pallas_call(
            functools.partial(kernel, sizes),
            out_shape=(out, out, lines, square, square),
            in_specs=[hbm] * 2,
            out_specs=[vmem] * 5,
            scratch_shapes=[
                pltpu.VMEM((planes, rows + 2 * PAD, columns), jnp.float32),
                pltpu.VMEM(mask.shape, jnp.int32),
                pltpu.VMEM((planes // CELLS, rows // CELLS + 16, columns), jnp.float32),
                pltpu.VMEM((2, planes, PAD, columns), jnp.float32),
                pltpu.VMEM((planes + 2 * RADIUS, rows, columns), jnp.float32),
                pltpu.VMEM((n_x, group, rows, columns), jnp.float32),
                pltpu.VMEM((rows, 128), jnp.float32),
                pltpu.VMEM((planes, 8, 128), jnp.float32),
                dma((5,)),
                dma((1,)),
                dma((chunks,)),
                dma((2,)),
                dma((2, chunks)),
                dma((2,)),
                dma((2,)),
                pltpu.SemaphoreType.REGULAR((2,)),
            ],
            compiler_params=pltpu.CompilerParams(
                collective_id=0, has_side_effects=True, vmem_limit_bytes=22 * 2**20
            ),
        )(*(pltpu.with_memory_space_constraint(a, pltpu.HBM) for a in (density, mask)))
        return pl.pallas_call(
            finish,
            out_shape=(out, out),
            in_specs=[vmem] * 5,
            out_specs=[hbm] * 2,
            scratch_shapes=[
                pltpu.VMEM((group, ROWS, columns * n_x), jnp.float32),
                pltpu.VMEM((group, ROWS, columns * n_x), jnp.float32),
                dma((2,)),
            ],
            compiler_params=pltpu.CompilerParams(vmem_limit_bytes=8 * 2**20),
        )(lines, near, far, filtered, projected)

    return jax.shard_map(
        body,
        mesh=mesh,
        in_specs=(P("gz", "gy", "gx"), P("gz", "gy", "gx")),
        out_specs=(P(("gz", "gx"), "gy", None), P(("gz", "gx"), "gy", None)),
        check_vma=False,
    )
```
